256 devices in a mesh: freq: 8 (over x_lo, y), src: 32 (over x_hi, z, core).
Axes of the slice: x: 4 (x_hi: 2, x_lo: 2; x = x_hi * 2 + x_lo), y: 4, z: 8, core: 2. Of those that a mesh axis runs over, the one named last changes fastest.
Arguments:
- recorded: float32 [4096, 512, 128], P('src', 'freq'), may hold values from -0.54 to 0.54
- panels: float32 [512, 512, 128], P('src', 'freq'), may hold values from -0.18 to 0.18
Outputs:
- multiples: float32 [4096, 512, 128], P('src', 'freq')
The draws below stay inside these ranges and needn't reach their ends.
All inputs are finite; a program needn't handle non-finite values.
Results may differ from the reference program's by a relative error of at most 0.00007.
Values sent between devices are 32-bit elements; how exact they have to be, the bound alone decides.
A program may use at most 128 MiB of HBM per device.

```python
import math
import jax
import jax.numpy as jnp
from jax import lax

K = 512
R = 512
NT = 128
NF = 64
SRC_DEV = 128
SOURCES = 4096


def levels(rng, extent, shards, low, largest):
    gain, own = 1.0, jax.random.fold_in(rng, 6)
    for axis_at, shards_of in shards:
        draws = jnp.exp(jax.random.uniform(jax.random.fold_in(own, axis_at), (shards_of,), jnp.float32, low / len(shards), largest / len(shards)))
        gain = gain * jnp.repeat(draws, extent[axis_at] // shards_of).reshape([-1 if axis == axis_at else 1 for axis in range(len(extent))])
    return gain


def gaussian(stream_key, extent, deviation, reach, shards=(), kind=jnp.bfloat16):
    values = deviation * jax.random.normal(stream_key, extent, jnp.float32)
    if shards:
        values = values * levels(stream_key, extent, shards, -0.22, 0.18)
    return jnp.clip(values, -reach, reach).astype(kind)


def setup_inputs(seed: int = 0) -> dict:
    streams_of = jax.random.split(jax.random.key(seed), 3)
    recorded = gaussian(streams_of[0], (SOURCES, K, NT), 0.09, 0.54, ((0, 32), (1, 8)), jnp.float32)
    panels = gaussian(streams_of[1], (K, R, NT), 0.03, 0.18, ((0, 32), (1, 8)), jnp.float32)
    return dict(recorded=recorded, panels=panels)


def lookup_tables(length, bins):
    freqs = jnp.arange(bins, dtype=jnp.int32)
    times = jnp.arange(length, dtype=jnp.int32)
    phase = (freqs[:, None] * times[None, :]) % length
    angle = (2.0 * math.pi / length) * phase.astype(jnp.float32)
    forward = jnp.stack([jnp.cos(angle), -jnp.sin(angle)], axis=1)
    weight = jnp.where(freqs == 0, 1.0, 2.0).astype(jnp.float32) / length
    inverse_transform = forward * weight[:, None, None]
    return forward, inverse_transform


def spectra(block, forward):
    return jnp.einsum('fct,abt->fcab', forward, block, precision=lax.Precision.HIGHEST)


def complex_product(left_operand, right_operand):
    upper_value = lax.Precision.HIGHEST
    real_part = jnp.einsum('vlx,vxp->vlp', left_operand[:, 0], right_operand[:, 0], precision=upper_value) - jnp.einsum('vlx,vxp->vlp', left_operand[:, 1], right_operand[:, 1], precision=upper_value)
    imaginary_part = jnp.einsum('vlx,vxp->vlp', left_operand[:, 0], right_operand[:, 1], precision=upper_value) + jnp.einsum('vlx,vxp->vlp', left_operand[:, 1], right_operand[:, 0], precision=upper_value)
    return jnp.stack([real_part, imaginary_part], axis=1)


def reference(recorded, panels):
    forward, inverse_transform = lookup_tables(NT, NF)
    panel_hat = spectra(panels, forward)
    blocks = recorded.reshape(SOURCES // SRC_DEV, SRC_DEV, K, NT)

    def one_block(block):
        predicted = complex_product(spectra(block, forward), panel_hat)
        return jnp.einsum('fcsr,fct->srt', predicted, inverse_transform, precision=lax.Precision.HIGHEST)

    result = lax.map(one_block, blocks)
    return result.reshape(SOURCES, R, NT)
```

```python
import functools

import jax
import jax.numpy as jnp
import numpy as np
from jax import lax
from jax.experimental import pallas as pl
from jax.experimental.pallas import tpu as pltpu
from jax.sharding import PartitionSpec as P

NT = 128
NF = 64
SLOTS = 4
MESH = pl.DeviceIdType.MESH
F32 = jnp.float32
BF16 = jnp.bfloat16

PLANE = [
    (1, 0), (0, 1), (3, 0), (0, 3), (1, 2), (2, 1), (3, 2), (2, 3),
    (1, 1), (3, 3), (2, 2), (1, 3), (3, 1), (2, 0), (0, 2),
]


def lookup_tables():
    phase = np.arange(NF)[:, None] * np.arange(NT)[None, :] % NT
    angle = 2.0 * np.pi / NT * phase
    forward = np.stack([np.cos(angle), -np.sin(angle)], axis=1)
    weight = np.where(np.arange(NF) == 0, 1.0, 2.0) / NT
    inverse = forward * weight[:, None, None]
    shape = (2 * NF, NT)
    return forward.reshape(shape).astype(np.float32), inverse.reshape(shape).astype(np.float32)


def split(value):
    high = value.astype(BF16)
    return high, (value - high.astype(F32)).astype(BF16)


def halves(first, second):
    lane = lax.broadcasted_iota(jnp.int32, first.shape, first.ndim - 1)
    low = jnp.where(lane < 64, first, pltpu.roll(second, 64, axis=first.ndim - 1))
    high = jnp.where(lane < 64, pltpu.roll(first, 64, axis=first.ndim - 1), second)
    return low, high


def kernel(
    rec_hbm, pan_hbm, fwd_ref, inv_ref, out_hbm,
    x_buf, p_buf, g_send, g_recv, g_all, d_send, d_recv, d_hi, d_lo, g_hi, g_lo, m_send, m_recv, o_buf,
    x_sem, p_sem, o_sem, gs_sem, gr_sem, ds_sem, dr_sem, ms_sem, mr_sem,
    fs_sem, fr_sem, bs_sem, br_sem, cs_sem, cr_sem,
):
    own_o = lax.axis_index("freq")
    src = lax.axis_index("src")
    own_xhi = src // 16
    zc = lax.rem(src, 16)
    z = zc // 2
    core = lax.rem(zc, 2)
    x = own_xhi * 2 + own_o // 4
    y = lax.rem(own_o, 4)
    own_q = own_xhi * 8 + own_o

    def plane(offset):
        px = lax.rem(x + offset[0], 4)
        py = lax.rem(y + offset[1], 4)
        o = lax.rem(px, 2) * 4 + py
        return o, px // 2

    def plane_id(offset):
        o, xhi = plane(offset)
        return (o, xhi * 16 + zc)

    step = 1 - 2 * core
    z_ahead = lax.rem(z + step + 8, 8)
    z_behind = lax.rem(z - step + 8, 8)
    ahead_id = (own_o, own_xhi * 16 + z_ahead * 2 + core)
    behind_id = (own_o, own_xhi * 16 + z_behind * 2 + core)
    partner_id = (own_o, own_xhi * 16 + z * 2 + 1 - core)

    pan_copy = pltpu.make_async_copy(pan_hbm, p_buf, p_sem)
    pan_copy.start()

    def rec_copy(chunk, half):
        rows = pl.ds(half * 64 + chunk * 16, 16)
        return pltpu.make_async_copy(rec_hbm.at[rows], x_buf.at[rows], x_sem.at[chunk, half])

    for chunk in range(4):
        for half in range(2):
            rec_copy(chunk, half).start()

    barrier = pltpu.get_barrier_semaphore()
    others = [plane_id(offset) for offset in PLANE] + [ahead_id, behind_id, partner_id]
    for other in others:
        pl.semaphore_signal(barrier, inc=1, device_id=other, device_id_type=MESH)

    nt = (((1,), (1,)), ((), ()))
    tn = (((0,), (0,)), ((), ()))

    pan_copy.wait()
    for kp in range(0, 8, 2):
        rows = jnp.concatenate([p_buf[kp], p_buf[kp + 8], p_buf[kp + 1], p_buf[kp + 9]], axis=0)
        hat = lax.dot_general(fwd_ref[...], rows, nt, precision=lax.Precision.HIGH, preferred_element_type=F32)
        g_send[pl.ds(kp, 128, stride=8), :] = hat[:, :128]
        g_send[pl.ds(kp + 1, 128, stride=8), :] = hat[:, 128:]

    pl.semaphore_wait(barrier, len(others))

    def g_copy(n):
        o, xhi = plane(PLANE[n])
        return pltpu.make_async_remote_copy(
            src_ref=g_send.at[pl.ds((xhi * 8 + o) * 64, 64)],
            dst_ref=g_recv.at[own_q],
            send_sem=gs_sem.at[n], recv_sem=gr_sem.at[n],
            device_id=plane_id(PLANE[n]), device_id_type=MESH,
        )

    for n in range(15):
        g_copy(n).start()
    g_recv[own_q] = g_send[pl.ds(own_q * 64, 64), :]

    for chunk in range(4):
        for half in range(2):
            rec_copy(chunk, half).wait()

        @pl.loop(0, 8)
        def _(pair):
            ih = chunk * 16 + pair * 2
            rows = jnp.concatenate([x_buf[ih], x_buf[ih + 64], x_buf[ih + 1], x_buf[ih + 65]], axis=0)
            hat = lax.dot_general(fwd_ref[...], rows, nt, precision=lax.Precision.HIGH, preferred_element_type=F32)
            d_send[pl.ds(ih, 128, stride=64), :] = hat[:, :128]
            d_send[pl.ds(ih + 1, 128, stride=64), :] = hat[:, 128:]

    def d_copy(slot, n):
        o, xhi = plane(PLANE[n])
        return pltpu.make_async_remote_copy(
            src_ref=d_send.at[pl.ds(((xhi * 8 + o) * SLOTS + slot) * 128, 128)],
            dst_ref=d_recv.at[slot, own_q],
            send_sem=ds_sem.at[slot, n], recv_sem=dr_sem.at[slot, n],
            device_id=plane_id(PLANE[n]), device_id_type=MESH,
        )

    @pl.loop(0, SLOTS)
    def _(slot):
        for n in range(15):
            d_copy(slot, n).start()

    @pl.loop(0, SLOTS)
    def _(slot):
        d_recv[slot, own_q] = d_send[pl.ds((own_q * SLOTS + slot) * 128, 128), :]

    for n in range(15):
        g_copy(n).wait_recv()

    @pl.loop(0, SLOTS)
    def _(slot):
        for c in range(2):
            rows = pl.ds((slot * 2 + c) * 8, 8)
            for xhi in range(2):
                for pair in range(4):
                    low, high = halves(g_recv[xhi * 8 + 2 * pair, rows, :], g_recv[xhi * 8 + 2 * pair + 1, rows, :])
                    g_all[slot, zc, c, xhi, 0:8, pair * 128:(pair + 1) * 128] = low
                    g_all[slot, zc, c, xhi, 8:16, pair * 128:(pair + 1) * 128] = high

    def block(hop, way):
        return lax.rem(z - way * hop * step + 32, 8) * 2 + core

    def ahead_copy(slot, hop):
        ref = g_all.at[slot, block(hop, 1)]
        return pltpu.make_async_remote_copy(
            src_ref=ref, dst_ref=ref, send_sem=fs_sem.at[slot, hop], recv_sem=fr_sem.at[slot, hop],
            device_id=ahead_id, device_id_type=MESH,
        )

    def behind_copy(slot, hop):
        ref = g_all.at[slot, block(hop, -1)]
        return pltpu.make_async_remote_copy(
            src_ref=ref, dst_ref=ref, send_sem=bs_sem.at[slot, hop], recv_sem=br_sem.at[slot, hop],
            device_id=behind_id, device_id_type=MESH,
        )

    def partner_copy(slot, n):
        ref = g_all.at[slot, block(n, 1) if n < 5 else block(n - 4, -1)]
        return pltpu.make_async_remote_copy(
            src_ref=ref, dst_ref=ref, send_sem=cs_sem.at[slot, n], recv_sem=cr_sem.at[slot, n],
            device_id=partner_id, device_id_type=MESH,
        )

    @pl.loop(0, SLOTS)
    def _(slot):
        ahead_copy(slot, 0).start()
        behind_copy(slot, 0).start()
        partner_copy(slot, 0).start()

    for hop in range(4):
        @pl.loop(0, SLOTS)
        def _(slot):
            ahead_copy(slot, hop).wait_recv()
            if hop < 3:
                ahead_copy(slot, hop + 1).start()
            partner_copy(slot, hop + 1).start()
            if hop < 3:
                behind_copy(slot, hop).wait_recv()
                if hop < 2:
                    behind_copy(slot, hop + 1).start()
                partner_copy(slot, hop + 5).start()

    def m_copy(slot, n):
        o, xhi = plane(PLANE[n])
        return pltpu.make_async_remote_copy(
            src_ref=m_send.at[slot, xhi * 8 + o],
            dst_ref=m_recv.at[pl.ds((own_q * SLOTS + slot) * 128, 128)],
            send_sem=ms_sem.at[slot, n], recv_sem=mr_sem.at[slot, n],
            device_id=plane_id(PLANE[n]), device_id_type=MESH,
        )

    def dot(left, right):
        return jnp.dot(left, right, preferred_element_type=F32)

    @pl.loop(0, SLOTS)
    def _(slot):
        for n in range(8):
            partner_copy(slot, n).wait_recv()

        @pl.loop(0, 16)
        def _(b):
            for c in range(2):
                for xhi in range(2):
                    high, low = split(g_all[slot, b, c, xhi])
                    rows = pl.ds(xhi * 256 + b * 16, 16)
                    g_hi[c, rows, :] = high
                    g_lo[c, rows, :] = low

        for n in range(15):
            d_copy(slot, n).wait_recv()

        for xhi in range(2):
            for pair in range(4):
                for c in range(2):
                    rows = pl.ds(c * 64, 64)
                    top, bottom = halves(
                        d_recv[slot, xhi * 8 + 2 * pair, rows, :], d_recv[slot, xhi * 8 + 2 * pair + 1, rows, :]
                    )
                    for at, part in ((0, top), (64, bottom)):
                        high, low = split(part)
                        d_hi[c, xhi * 128 + at:xhi * 128 + at + 64, pair * 128:(pair + 1) * 128] = high
                        d_lo[c, xhi * 128 + at:xhi * 128 + at + 64, pair * 128:(pair + 1) * 128] = low

        @pl.loop(0, 2)
        def _(xhi):
            rows = pl.ds(xhi * 128, 128)
            for tile in range(2):
                cols = slice(tile * 256, (tile + 1) * 256)

                def product(a, b):
                    return (
                        dot(d_hi[a, rows, :], g_hi[b, :, cols])
                        + dot(d_hi[a, rows, :], g_lo[b, :, cols])
                        + dot(d_lo[a, rows, :], g_hi[b, :, cols])
                    )

                real = product(0, 0) - product(1, 1)
                imag = product(0, 1) + product(1, 0)
                for c, value in ((0, real), (1, imag)):
                    for lanes in range(2):
                        part = value[:, lanes * 128:(lanes + 1) * 128]
                        even, odd = halves(part[:64], part[64:])
                        o = tile * 4 + lanes * 2
                        m_send[slot, xhi * 8 + o, c * 64:(c + 1) * 64, :] = even
                        m_send[slot, xhi * 8 + o + 1, c * 64:(c + 1) * 64, :] = odd

        for n in range(15):
            m_copy(slot, n).start()
        m_recv[pl.ds((own_q * SLOTS + slot) * 128, 128), :] = m_send[slot, own_q]

    @pl.loop(0, SLOTS)
    def _(slot):
        for n in range(15):
            m_copy(slot, n).wait_recv()

    def out_copy(chunk, half):
        rows = pl.ds(half * 64 + chunk * 16, 16)
        return pltpu.make_async_copy(o_buf.at[rows], out_hbm.at[rows], o_sem.at[chunk, half])

    for chunk in range(4):
        @pl.loop(0, 8)
        def _(pair):
            for u in range(2):
                ih = chunk * 16 + pair * 2 + u
                part = m_recv[pl.ds(ih, 128, stride=64), :]
                value = lax.dot_general(part, inv_ref[...], tn, precision=lax.Precision.HIGH, preferred_element_type=F32)
                o_buf[ih] = value[:64]
                o_buf[ih + 64] = value[64:]

        for half in range(2):
            out_copy(chunk, half).start()

    for n in range(15):
        g_copy(n).wait_send()

    @pl.loop(0, SLOTS)
    def _(slot):
        for n in range(15):
            d_copy(slot, n).wait_send()
            m_copy(slot, n).wait_send()
        for hop in range(4):
            ahead_copy(slot, hop).wait_send()
        for hop in range(3):
            behind_copy(slot, hop).wait_send()
        for n in range(8):
            partner_copy(slot, n).wait_send()

    for chunk in range(4):
        for half in range(2):
            out_copy(chunk, half).wait()


def local(recorded, panels):
    forward, inverse = lookup_tables()
    dma = pltpu.SemaphoreType.DMA
    return pl.pallas_call(
        kernel,
        out_shape=jax.ShapeDtypeStruct((128, 64, NT), F32),
        in_specs=[
            pl.BlockSpec(memory_space=pl.ANY),
            pl.BlockSpec(memory_space=pl.ANY),
            pl.BlockSpec(memory_space=pltpu.VMEM),
            pl.BlockSpec(memory_space=pltpu.VMEM),
        ],
        out_specs=pl.BlockSpec(memory_space=pl.ANY),
        scratch_shapes=[
            pltpu.VMEM((128, 64, NT), F32),
            pltpu.VMEM((16, 64, NT), F32),
            pltpu.VMEM((1024, 128), F32),
            pltpu.VMEM((16, 64, 128), F32),
            pltpu.VMEM((SLOTS, 16, 2, 2, 16, 512), F32),
            pltpu.VMEM((8192, 128), F32),
            pltpu.VMEM((SLOTS, 16, 128, 128), F32),
            pltpu.VMEM((2, 256, 512), BF16),
            pltpu.VMEM((2, 256, 512), BF16),
            pltpu.VMEM((2, 512, 512), BF16),
            pltpu.VMEM((2, 512, 512), BF16),
            pltpu.VMEM((SLOTS, 16, 128, 128), F32),
            pltpu.VMEM((8192, 128), F32),
            pltpu.VMEM((128, 64, NT), F32),
            dma((4, 2)), dma, dma((4, 2)),
            dma((15,)), dma((15,)),
            dma((SLOTS, 15)), dma((SLOTS, 15)),
            dma((SLOTS, 15)), dma((SLOTS, 15)),
            dma((SLOTS, 4)), dma((SLOTS, 4)),
            dma((SLOTS, 3)), dma((SLOTS, 3)),
            dma((SLOTS, 8)), dma((SLOTS, 8)),
        ],
        compiler_params=pltpu.CompilerParams(
            collective_id=0, has_side_effects=True, vmem_limit_bytes=56 * 1024 * 1024
        ),
        name="convolve",
    )(recorded, panels, jnp.asarray(forward), jnp.asarray(inverse))


def solution(mesh):
    return jax.shard_map(
        local,
        mesh=mesh,
        in_specs=(P("src", "freq", None), P("src", "freq", None)),
        out_specs=P("src", "freq", None),
        check_vma=False,
    )
```

```python
import functools

import jax
import jax.numpy as jnp
import numpy as np
from jax import lax
from jax.experimental import pallas as pl
from jax.experimental.pallas import tpu as pltpu
from jax.sharding import PartitionSpec as P

NT = 128
NF = 64
SLOTS = 4
MESH = pl.DeviceIdType.MESH
F32 = jnp.float32
BF16 = jnp.bfloat16

PLANE = [
    (1, 0), (0, 1), (3, 0), (0, 3), (1, 2), (2, 1), (3, 2), (2, 3),
    (1, 1), (3, 3), (2, 2), (1, 3), (3, 1), (2, 0), (0, 2),
]


def lookup_tables():
    phase = np.arange(NF)[:, None] * np.arange(NT)[None, :] % NT
    angle = 2.0 * np.pi / NT * phase
    forward = np.stack([np.cos(angle), -np.sin(angle)], axis=1)
    weight = np.where(np.arange(NF) == 0, 1.0, 2.0) / NT
    inverse = forward * weight[:, None, None]
    forward = forward.reshape(2 * NF, NT)
    inverse = inverse.reshape(16, SLOTS, 2, NT).transpose(1, 0, 2, 3).reshape(2 * NF, NT)
    return [np.asarray(part) for table in (forward, inverse) for part in split_table(table)]


def split_table(table):
    high = table.astype(np.float32).astype(BF16)
    low = (table - high.astype(np.float64)).astype(np.float32).astype(BF16)
    return high, low


def split(value):
    high = value.astype(BF16)
    return high, (value - high.astype(F32)).astype(BF16)


def halves(first, second):
    lane = lax.broadcasted_iota(jnp.int32, first.shape, first.ndim - 1)
    low = jnp.where(lane < 64, first, pltpu.roll(second, 64, axis=first.ndim - 1))
    high = jnp.where(lane < 64, pltpu.roll(first, 64, axis=first.ndim - 1), second)
    return low, high


def kernel(
    rec_hbm, pan_hbm, fwd_hi, fwd_lo, inv_hi, inv_lo, acc_ref, m_last,
    x_buf, p_buf, g_send, g_recv, g_all, d_send, d_recv, d_hi, d_lo, g_hi, g_lo, m_send, m_recv,
    x_sem, p_sem, gs_sem, gr_sem, ds_sem, dr_sem, ms_sem, mr_sem,
    fs_sem, fr_sem, bs_sem, br_sem, cs_sem, cr_sem,
):
    own_o = lax.axis_index("freq")
    src = lax.axis_index("src")
    own_xhi = src // 16
    zc = lax.rem(src, 16)
    z = zc // 2
    core = lax.rem(zc, 2)
    x = own_xhi * 2 + own_o // 4
    y = lax.rem(own_o, 4)
    own_q = own_xhi * 8 + own_o

    def plane(offset):
        px = lax.rem(x + offset[0], 4)
        py = lax.rem(y + offset[1], 4)
        o = lax.rem(px, 2) * 4 + py
        return o, px // 2

    def plane_id(offset):
        o, xhi = plane(offset)
        return (o, xhi * 16 + zc)

    step = 1 - 2 * core
    z_ahead = lax.rem(z + step + 8, 8)
    z_behind = lax.rem(z - step + 8, 8)
    ahead_id = (own_o, own_xhi * 16 + z_ahead * 2 + core)
    behind_id = (own_o, own_xhi * 16 + z_behind * 2 + core)
    partner_id = (own_o, own_xhi * 16 + z * 2 + 1 - core)

    pan_copy = pltpu.make_async_copy(pan_hbm, p_buf, p_sem)
    pan_copy.start()

    def rec_copy(chunk, half):
        rows = pl.ds(half * 64 + chunk * 16, 16)
        return pltpu.make_async_copy(rec_hbm.at[rows], x_buf.at[rows], x_sem.at[chunk, half])

    for chunk in range(4):
        for half in range(2):
            rec_copy(chunk, half).start()

    barrier = pltpu.get_barrier_semaphore()
    others = [plane_id(offset) for offset in PLANE] + [ahead_id, behind_id, partner_id]
    for other in others:
        pl.semaphore_signal(barrier, inc=1, device_id=other, device_id_type=MESH)

    nt = (((1,), (1,)), ((), ()))

    def forward(rows):
        high, low = split(rows)
        return (
            lax.dot_general(fwd_hi[...], high, nt, preferred_element_type=F32)
            + lax.dot_general(fwd_hi[...], low, nt, preferred_element_type=F32)
            + lax.dot_general(fwd_lo[...], high, nt, preferred_element_type=F32)
        )

    pan_copy.wait()
    for kp in range(0, 8, 2):
        rows = jnp.concatenate([p_buf[kp], p_buf[kp + 8], p_buf[kp + 1], p_buf[kp + 9]], axis=0)
        hat = forward(rows)
        g_send[pl.ds(kp, 128, stride=8), :] = hat[:, :128]
        g_send[pl.ds(kp + 1, 128, stride=8), :] = hat[:, 128:]

    pl.semaphore_wait(barrier, len(others))

    def g_copy(n):
        o, xhi = plane(PLANE[n])
        return pltpu.make_async_remote_copy(
            src_ref=g_send.at[pl.ds((xhi * 8 + o) * 64, 64)],
            dst_ref=g_recv.at[own_q],
            send_sem=gs_sem.at[n], recv_sem=gr_sem.at[n],
            device_id=plane_id(PLANE[n]), device_id_type=MESH,
        )

    for n in range(15):
        g_copy(n).start()
    g_recv[own_q] = g_send[pl.ds(own_q * 64, 64), :]

    for chunk in range(4):
        for half in range(2):
            rec_copy(chunk, half).wait()

        @pl.loop(0, 8)
        def _(pair):
            ih = chunk * 16 + pair * 2
            rows = jnp.concatenate([x_buf[ih], x_buf[ih + 64], x_buf[ih + 1], x_buf[ih + 65]], axis=0)
            hat = forward(rows)
            d_send[pl.ds(ih, 128, stride=64), :] = hat[:, :128]
            d_send[pl.ds(ih + 1, 128, stride=64), :] = hat[:, 128:]

    def d_copy(slot, n):
        o, xhi = plane(PLANE[n])
        return pltpu.make_async_remote_copy(
            src_ref=d_send.at[pl.ds(((xhi * 8 + o) * SLOTS + slot) * 128, 128)],
            dst_ref=d_recv.at[slot, own_q],
            send_sem=ds_sem.at[slot, n], recv_sem=dr_sem.at[slot, n],
            device_id=plane_id(PLANE[n]), device_id_type=MESH,
        )

    @pl.loop(0, SLOTS)
    def _(slot):
        for n in range(15):
            d_copy(slot, n).start()

    @pl.loop(0, SLOTS)
    def _(slot):
        d_recv[slot, own_q] = d_send[pl.ds((own_q * SLOTS + slot) * 128, 128), :]

    for n in range(15):
        g_copy(n).wait_recv()

    @pl.loop(0, SLOTS)
    def _(slot):
        for c in range(2):
            rows = pl.ds((slot * 2 + c) * 8, 8)
            for xhi in range(2):
                for pair in range(4):
                    low, high = halves(g_recv[xhi * 8 + 2 * pair, rows, :], g_recv[xhi * 8 + 2 * pair + 1, rows, :])
                    g_all[slot, zc, c, xhi, 0:8, pair * 128:(pair + 1) * 128] = low
                    g_all[slot, zc, c, xhi, 8:16, pair * 128:(pair + 1) * 128] = high

    def block(hop, way):
        return lax.rem(z - way * hop * step + 32, 8) * 2 + core

    def ahead_copy(slot, hop):
        ref = g_all.at[slot, block(hop, 1)]
        return pltpu.make_async_remote_copy(
            src_ref=ref, dst_ref=ref, send_sem=fs_sem.at[slot, hop], recv_sem=fr_sem.at[slot, hop],
            device_id=ahead_id, device_id_type=MESH,
        )

    def behind_copy(slot, hop):
        ref = g_all.at[slot, block(hop, -1)]
        return pltpu.make_async_remote_copy(
            src_ref=ref, dst_ref=ref, send_sem=bs_sem.at[slot, hop], recv_sem=br_sem.at[slot, hop],
            device_id=behind_id, device_id_type=MESH,
        )

    def partner_copy(slot, n):
        ref = g_all.at[slot, block(n, 1) if n < 5 else block(n - 4, -1)]
        return pltpu.make_async_remote_copy(
            src_ref=ref, dst_ref=ref, send_sem=cs_sem.at[slot, n], recv_sem=cr_sem.at[slot, n],
            device_id=partner_id, device_id_type=MESH,
        )

    @pl.loop(0, SLOTS)
    def _(slot):
        ahead_copy(slot, 0).start()
        behind_copy(slot, 0).start()
        partner_copy(slot, 0).start()

    for hop in range(4):
        @pl.loop(0, SLOTS)
        def _(slot):
            ahead_copy(slot, hop).wait_recv()
            if hop < 3:
                ahead_copy(slot, hop + 1).start()
            partner_copy(slot, hop + 1).start()
            if hop < 3:
                behind_copy(slot, hop).wait_recv()
                if hop < 2:
                    behind_copy(slot, hop + 1).start()
                partner_copy(slot, hop + 5).start()

    def m_copy(slot, n):
        o, xhi = plane(PLANE[n])
        if slot is None:
            slot, dst = SLOTS - 1, m_last
        else:
            dst = m_recv.at[slot]
        return pltpu.make_async_remote_copy(
            src_ref=m_send.at[slot, xhi * 8 + o],
            dst_ref=dst.at[pl.ds(own_q * 128, 128)],
            send_sem=ms_sem.at[slot, n], recv_sem=mr_sem.at[slot, n],
            device_id=plane_id(PLANE[n]), device_id_type=MESH,
        )

    def dot(left, right):
        return jnp.dot(left, right, preferred_element_type=F32)

    def predict(slot):
        for n in range(8):
            partner_copy(slot, n).wait_recv()

        @pl.loop(0, 16)
        def _(b):
            for c in range(2):
                for xhi in range(2):
                    high, low = split(g_all[slot, b, c, xhi])
                    rows = pl.ds(xhi * 256 + b * 16, 16)
                    g_hi[c, rows, :] = high
                    g_lo[c, rows, :] = low

        for n in range(15):
            d_copy(slot, n).wait_recv()

        for xhi in range(2):
            for pair in range(4):
                for c in range(2):
                    rows = pl.ds(c * 64, 64)
                    top, bottom = halves(
                        d_recv[slot, xhi * 8 + 2 * pair, rows, :], d_recv[slot, xhi * 8 + 2 * pair + 1, rows, :]
                    )
                    for at, part in ((0, top), (64, bottom)):
                        high, low = split(part)
                        d_hi[c, xhi * 128 + at:xhi * 128 + at + 64, pair * 128:(pair + 1) * 128] = high
                        d_lo[c, xhi * 128 + at:xhi * 128 + at + 64, pair * 128:(pair + 1) * 128] = low

        @pl.loop(0, 2)
        def _(xhi):
            rows = pl.ds(xhi * 128, 128)
            for tile in range(2):
                cols = slice(tile * 256, (tile + 1) * 256)

                def product(a, b):
                    return (
                        dot(d_hi[a, rows, :], g_hi[b, :, cols])
                        + dot(d_hi[a, rows, :], g_lo[b, :, cols])
                        + dot(d_lo[a, rows, :], g_hi[b, :, cols])
                    )

                real = product(0, 0) - product(1, 1)
                imag = product(0, 1) + product(1, 0)
                for c, value in ((0, real), (1, imag)):
                    for lanes in range(2):
                        part = value[:, lanes * 128:(lanes + 1) * 128]
                        even, odd = halves(part[:64], part[64:])
                        o = tile * 4 + lanes * 2
                        m_send[slot, xhi * 8 + o, c * 64:(c + 1) * 64, :] = even
                        m_send[slot, xhi * 8 + o + 1, c * 64:(c + 1) * 64, :] = odd

    @pl.loop(0, SLOTS - 1)
    def _(slot):
        predict(slot)
        for n in range(15):
            m_copy(slot, n).start()
        m_recv[slot, pl.ds(own_q * 128, 128), :] = m_send[slot, own_q]

    predict(SLOTS - 1)
    for n in range(15):
        m_copy(None, n).start()
    m_last[pl.ds(own_q * 128, 128), :] = m_send[SLOTS - 1, own_q]

    @pl.loop(0, SLOTS - 1)
    def _(slot):
        for n in range(15):
            m_copy(slot, n).wait_recv()

    @pl.loop(0, 32)
    def _(pair):
        for u in range(2):
            ih = pair * 2 + u
            part = jnp.concatenate([m_recv[slot, pl.ds(ih, 32, stride=64), :] for slot in range(SLOTS - 1)], axis=0)
            high, low = split(part.T)
            value = dot(high, inv_hi[0:96]) + dot(low, inv_hi[0:96]) + dot(high, inv_lo[0:96])
            acc_ref[ih] = value[:64]
            acc_ref[ih + 64] = value[64:]

    for n in range(15):
        m_copy(None, n).wait_recv()

    for n in range(15):
        g_copy(n).wait_send()

    @pl.loop(0, SLOTS)
    def _(slot):
        for n in range(15):
            d_copy(slot, n).wait_send()
        for hop in range(4):
            ahead_copy(slot, hop).wait_send()
        for hop in range(3):
            behind_copy(slot, hop).wait_send()
        for n in range(8):
            partner_copy(slot, n).wait_send()

    @pl.loop(0, SLOTS - 1)
    def _(slot):
        for n in range(15):
            m_copy(slot, n).wait_send()

    for n in range(15):
        m_copy(None, n).wait_send()


def finish(acc_ref, m_last, inv_hi, inv_lo, out_ref):
    first = pl.program_id(0) * 8
    table_hi = inv_hi[96:128]
    table_lo = inv_lo[96:128]
    for u in range(8):
        part = m_last[pl.ds(first + u, 32, stride=64), :]
        high, low = split(part.T)
        value = (
            jnp.dot(high, table_hi, preferred_element_type=F32)
            + jnp.dot(low, table_hi, preferred_element_type=F32)
            + jnp.dot(high, table_lo, preferred_element_type=F32)
        )
        out_ref[0, u] = acc_ref[0, first + u] + value[:64]
        out_ref[1, u] = acc_ref[1, first + u] + value[64:]


def local(recorded, panels):
    tables = [jnp.asarray(table) for table in lookup_tables()]
    dma = pltpu.SemaphoreType.DMA
    whole = pl.BlockSpec(memory_space=pltpu.VMEM)
    acc, last = pl.pallas_call(
        kernel,
        out_shape=(pltpu.VMEM((128, 64, NT), F32), pltpu.VMEM((2048, 128), F32)),
        in_specs=[
            pl.BlockSpec(memory_space=pl.ANY),
            pl.BlockSpec(memory_space=pl.ANY),
            whole, whole, whole, whole,
        ],
        out_specs=(whole, whole),
        scratch_shapes=[
            pltpu.VMEM((128, 64, NT), F32),
            pltpu.VMEM((16, 64, NT), F32),
            pltpu.VMEM((1024, 128), F32),
            pltpu.VMEM((16, 64, 128), F32),
            pltpu.VMEM((SLOTS, 16, 2, 2, 16, 512), F32),
            pltpu.VMEM((8192, 128), F32),
            pltpu.VMEM((SLOTS, 16, 128, 128), F32),
            pltpu.VMEM((2, 256, 512), BF16),
            pltpu.VMEM((2, 256, 512), BF16),
            pltpu.VMEM((2, 512, 512), BF16),
            pltpu.VMEM((2, 512, 512), BF16),
            pltpu.VMEM((SLOTS, 16, 128, 128), F32),
            pltpu.VMEM((SLOTS - 1, 2048, 128), F32),
            dma((4, 2)), dma,
            dma((15,)), dma((15,)),
            dma((SLOTS, 15)), dma((SLOTS, 15)),
            dma((SLOTS, 15)), dma((SLOTS, 15)),
            dma((SLOTS, 4)), dma((SLOTS, 4)),
            dma((SLOTS, 3)), dma((SLOTS, 3)),
            dma((SLOTS, 8)), dma((SLOTS, 8)),
        ],
        compiler_params=pltpu.CompilerParams(
            collective_id=0, has_side_effects=True, vmem_limit_bytes=50 * 1024 * 1024
        ),
        name="convolve",
    )(recorded, panels, *tables)
    out = pl.pallas_call(
        finish,
        grid=(8,),
        out_shape=jax.ShapeDtypeStruct((2, 64, 64, NT), F32),
        in_specs=[whole, whole, whole, whole],
        out_specs=pl.BlockSpec((2, 8, 64, NT), lambda g: (0, g, 0, 0)),
        compiler_params=pltpu.CompilerParams(vmem_limit_bytes=16 * 1024 * 1024),
        name="finish",
    )(acc.reshape(2, 64, 64, NT), last, tables[2], tables[3])
    return out.reshape(128, 64, NT)


def solution(mesh):
    return jax.shard_map(
        local,
        mesh=mesh,
        in_specs=(P("src", "freq", None), P("src", "freq", None)),
        out_specs=P("src", "freq", None),
        check_vma=False,
    )
```

```python
import functools

import jax
import jax.numpy as jnp
import numpy as np
from jax import lax
from jax.experimental import pallas as pl
from jax.experimental.pallas import tpu as pltpu
from jax.sharding import PartitionSpec as P

NT = 128
NF = 64
SLOTS = 4
PITCH = 72
MESH = pl.DeviceIdType.MESH
F32 = jnp.float32
BF16 = jnp.bfloat16

PLANE = [
    (1, 0), (0, 1), (3, 0), (0, 3), (1, 2), (2, 1), (3, 2), (2, 3),
    (1, 1), (3, 3), (2, 2), (1, 3), (3, 1), (2, 0), (0, 2),
]


def lookup_tables():
    phase = np.arange(NF)[:, None] * np.arange(NT)[None, :] % NT
    angle = 2.0 * np.pi / NT * phase
    forward = np.stack([np.cos(angle), -np.sin(angle)], axis=1)
    weight = np.where(np.arange(NF) == 0, 1.0, 2.0) / NT
    inverse = forward * weight[:, None, None]
    forward = forward.reshape(2 * NF, NT)
    inverse = inverse.reshape(16, SLOTS, 2, NT).transpose(1, 0, 2, 3).reshape(2 * NF, NT)
    tables = [np.asarray(part) for table in (forward, inverse) for part in split_table(table)]
    tail_hi, tail_lo = (np.kron(np.eye(4), part[96:].astype(np.float32)).astype(BF16) for part in tables[2:])
    return tables, (np.concatenate([tail_hi, tail_hi]), tail_lo)


def split_table(table):
    high = table.astype(np.float32).astype(BF16)
    low = (table - high.astype(np.float64)).astype(np.float32).astype(BF16)
    return high, low


def split(value):
    high = value.astype(BF16)
    return high, (value - high.astype(F32)).astype(BF16)


def halves(first, second):
    lane = lax.broadcasted_iota(jnp.int32, first.shape, first.ndim - 1)
    low = jnp.where(lane < 64, first, pltpu.roll(second, 64, axis=first.ndim - 1))
    high = jnp.where(lane < 64, pltpu.roll(first, 64, axis=first.ndim - 1), second)
    return low, high


def kernel(
    rec_hbm, pan_hbm, fwd_hi, fwd_lo, inv_hi, inv_lo, acc_ref, m_last,
    x_buf, p_buf, g_send, g_recv, g_all, d_send, d_recv, d_hi, d_lo, g_hi, g_lo, m_send, m_recv,
    x_sem, p_sem, gs_sem, gr_sem, ds_sem, dr_sem, ms_sem, mr_sem,
    fs_sem, fr_sem, bs_sem, br_sem, cs_sem, cr_sem,
):
    own_o = lax.axis_index("freq")
    src = lax.axis_index("src")
    own_xhi = src // 16
    zc = lax.rem(src, 16)
    z = zc // 2
    core = lax.rem(zc, 2)
    x = own_xhi * 2 + own_o // 4
    y = lax.rem(own_o, 4)
    own_q = own_xhi * 8 + own_o

    def plane(offset):
        px = lax.rem(x + offset[0], 4)
        py = lax.rem(y + offset[1], 4)
        o = lax.rem(px, 2) * 4 + py
        return o, px // 2

    def plane_id(offset):
        o, xhi = plane(offset)
        return (o, xhi * 16 + zc)

    step = 1 - 2 * core
    z_ahead = lax.rem(z + step + 8, 8)
    z_behind = lax.rem(z - step + 8, 8)
    ahead_id = (own_o, own_xhi * 16 + z_ahead * 2 + core)
    behind_id = (own_o, own_xhi * 16 + z_behind * 2 + core)
    partner_id = (own_o, own_xhi * 16 + z * 2 + 1 - core)

    pan_copy = pltpu.make_async_copy(pan_hbm, p_buf, p_sem)
    pan_copy.start()

    def rec_copy(chunk, half):
        rows = pl.ds(half * 64 + chunk * 16, 16)
        return pltpu.make_async_copy(rec_hbm.at[rows], x_buf.at[rows], x_sem.at[chunk, half])

    for chunk in range(4):
        for half in range(2):
            rec_copy(chunk, half).start()

    barrier = pltpu.get_barrier_semaphore()
    others = [plane_id(offset) for offset in PLANE] + [ahead_id, behind_id, partner_id]
    for other in others:
        pl.semaphore_signal(barrier, inc=1, device_id=other, device_id_type=MESH)

    nt = (((1,), (1,)), ((), ()))

    def forward(rows):
        high, low = split(rows)
        return (
            lax.dot_general(fwd_hi[...], high, nt, preferred_element_type=F32)
            + lax.dot_general(fwd_hi[...], low, nt, preferred_element_type=F32)
            + lax.dot_general(fwd_lo[...], high, nt, preferred_element_type=F32)
        )

    pan_copy.wait()
    for kp in range(0, 8, 2):
        rows = jnp.concatenate([p_buf[kp], p_buf[kp + 8], p_buf[kp + 1], p_buf[kp + 9]], axis=0)
        hat = forward(rows)
        g_send[pl.ds(kp, 128, stride=8), :] = hat[:, :128]
        g_send[pl.ds(kp + 1, 128, stride=8), :] = hat[:, 128:]

    pl.semaphore_wait(barrier, len(others))

    def g_copy(n):
        o, xhi = plane(PLANE[n])
        return pltpu.make_async_remote_copy(
            src_ref=g_send.at[pl.ds((xhi * 8 + o) * 64, 64)],
            dst_ref=g_recv.at[own_q],
            send_sem=gs_sem.at[n], recv_sem=gr_sem.at[n],
            device_id=plane_id(PLANE[n]), device_id_type=MESH,
        )

    for n in range(15):
        g_copy(n).start()
    g_recv[own_q] = g_send[pl.ds(own_q * 64, 64), :]

    for chunk in range(4):
        for half in range(2):
            rec_copy(chunk, half).wait()

        @pl.loop(0, 8)
        def _(pair):
            ih = chunk * 16 + pair * 2
            rows = jnp.concatenate([x_buf[ih], x_buf[ih + 64], x_buf[ih + 1], x_buf[ih + 65]], axis=0)
            hat = forward(rows)
            d_send[:, ih, :] = hat[:, :128]
            d_send[:, ih + 1, :] = hat[:, 128:]

    def d_copy(slot, n):
        o, xhi = plane(PLANE[n])
        return pltpu.make_async_remote_copy(
            src_ref=d_send.at[pl.ds(((xhi * 8 + o) * SLOTS + slot) * 2, 2), pl.ds(0, 64)],
            dst_ref=d_recv.at[slot, own_q],
            send_sem=ds_sem.at[slot, n], recv_sem=dr_sem.at[slot, n],
            device_id=plane_id(PLANE[n]), device_id_type=MESH,
        )

    @pl.loop(0, SLOTS)
    def _(slot):
        for n in range(15):
            d_copy(slot, n).start()

    @pl.loop(0, SLOTS)
    def _(slot):
        d_recv[slot, own_q] = d_send[pl.ds((own_q * SLOTS + slot) * 2, 2), 0:64, :]

    for n in range(15):
        g_copy(n).wait_recv()

    @pl.loop(0, SLOTS)
    def _(slot):
        for c in range(2):
            rows = pl.ds((slot * 2 + c) * 8, 8)
            for xhi in range(2):
                for pair in range(4):
                    low, high = halves(g_recv[xhi * 8 + 2 * pair, rows, :], g_recv[xhi * 8 + 2 * pair + 1, rows, :])
                    g_all[slot, zc, c, xhi, 0:8, pair * 128:(pair + 1) * 128] = low
                    g_all[slot, zc, c, xhi, 8:16, pair * 128:(pair + 1) * 128] = high

    def block(hop, way):
        return lax.rem(z - way * hop * step + 32, 8) * 2 + core

    def ahead_copy(slot, hop):
        ref = g_all.at[slot, block(hop, 1)]
        return pltpu.make_async_remote_copy(
            src_ref=ref, dst_ref=ref, send_sem=fs_sem.at[slot, hop], recv_sem=fr_sem.at[slot, hop],
            device_id=ahead_id, device_id_type=MESH,
        )

    def behind_copy(slot, hop):
        ref = g_all.at[slot, block(hop, -1)]
        return pltpu.make_async_remote_copy(
            src_ref=ref, dst_ref=ref, send_sem=bs_sem.at[slot, hop], recv_sem=br_sem.at[slot, hop],
            device_id=behind_id, device_id_type=MESH,
        )

    def partner_copy(slot, n):
        ref = g_all.at[slot, block(n, 1) if n < 5 else block(n - 4, -1)]
        return pltpu.make_async_remote_copy(
            src_ref=ref, dst_ref=ref, send_sem=cs_sem.at[slot, n], recv_sem=cr_sem.at[slot, n],
            device_id=partner_id, device_id_type=MESH,
        )

    def first(slot):
        ahead_copy(slot, 0).start()
        behind_copy(slot, 0).start()
        partner_copy(slot, 0).start()

    def pass_on(hop, slot):
        ahead_copy(slot, hop).wait_recv()
        if hop < 3:
            ahead_copy(slot, hop + 1).start()
        partner_copy(slot, hop + 1).start()
        if hop < 3:
            behind_copy(slot, hop).wait_recv()
            if hop < 2:
                behind_copy(slot, hop + 1).start()
            partner_copy(slot, hop + 5).start()

    first(0)
    first(1)
    pass_on(0, 0)
    first(2)
    pass_on(1, 0)
    pass_on(0, 1)
    first(3)
    pass_on(2, 0)
    pass_on(1, 1)
    pass_on(0, 2)

    def m_copy(slot, n):
        o, xhi = plane(PLANE[n])
        if slot is None:
            slot, dst = SLOTS - 1, m_last
        else:
            dst = m_recv.at[slot]
        return pltpu.make_async_remote_copy(
            src_ref=m_send.at[slot, xhi * 8 + o],
            dst_ref=dst.at[pl.ds(own_q * 2, 2), pl.ds(0, 64)],
            send_sem=ms_sem.at[slot, n], recv_sem=mr_sem.at[slot, n],
            device_id=plane_id(PLANE[n]), device_id_type=MESH,
        )

    def dot(left, right):
        return jnp.dot(left, right, preferred_element_type=F32)

    def predict(slot):
        for n in range(8):
            partner_copy(slot, n).wait_recv()

        @pl.loop(0, 16)
        def _(b):
            for c in range(2):
                for xhi in range(2):
                    high, low = split(g_all[slot, b, c, xhi])
                    rows = pl.ds(xhi * 256 + b * 16, 16)
                    g_hi[c, rows, :] = high
                    g_lo[c, rows, :] = low

        for n in range(15):
            d_copy(slot, n).wait_recv()

        for xhi in range(2):
            for pair in range(4):
                for c in range(2):
                    top, bottom = halves(
                        d_recv[slot, xhi * 8 + 2 * pair, c], d_recv[slot, xhi * 8 + 2 * pair + 1, c]
                    )
                    for at, part in ((0, top), (64, bottom)):
                        high, low = split(part)
                        d_hi[c, xhi * 128 + at:xhi * 128 + at + 64, pair * 128:(pair + 1) * 128] = high
                        d_lo[c, xhi * 128 + at:xhi * 128 + at + 64, pair * 128:(pair + 1) * 128] = low

        @pl.loop(0, 2)
        def _(xhi):
            rows = pl.ds(xhi * 128, 128)
            for tile in range(2):
                cols = slice(tile * 256, (tile + 1) * 256)

                def product(a, b):
                    return (
                        dot(d_hi[a, rows, :], g_hi[b, :, cols])
                        + dot(d_hi[a, rows, :], g_lo[b, :, cols])
                        + dot(d_lo[a, rows, :], g_hi[b, :, cols])
                    )

                real = product(0, 0) - product(1, 1)
                imag = product(0, 1) + product(1, 0)
                for c, value in ((0, real), (1, imag)):
                    for lanes in range(2):
                        part = value[:, lanes * 128:(lanes + 1) * 128]
                        even, odd = halves(part[:64], part[64:])
                        o = tile * 4 + lanes * 2
                        m_send[slot, xhi * 8 + o, c] = even
                        m_send[slot, xhi * 8 + o + 1, c] = odd

    @pl.loop(0, SLOTS - 1)
    def _(slot):
        pass_on(3, slot)
        pass_on(2, slot + 1)

        @pl.when(slot < 2)
        def _():
            pass_on(1, slot + 2)

        @pl.when(slot < 1)
        def _():
            pass_on(0, slot + 3)

        predict(slot)
        for n in range(15):
            m_copy(slot, n).start()
        m_recv[slot, pl.ds(own_q * 2, 2), 0:64, :] = m_send[slot, own_q]

    pass_on(3, SLOTS - 1)
    predict(SLOTS - 1)
    for n in range(15):
        m_copy(None, n).start()
    m_last[pl.ds(own_q * 2, 2), 0:64, :] = m_send[SLOTS - 1, own_q]

    @pl.loop(0, SLOTS - 1)
    def _(slot):
        for n in range(15):
            m_copy(slot, n).wait_recv()

    @pl.loop(0, 32)
    def _(pair):
        for u in range(2):
            ih = pair * 2 + u
            part = jnp.concatenate([m_recv[slot, :, ih, :] for slot in range(SLOTS - 1)], axis=0)
            high, low = split(part.T)
            value = dot(high, inv_hi[0:96]) + dot(low, inv_hi[0:96]) + dot(high, inv_lo[0:96])
            acc_ref[ih] = value[:64]
            acc_ref[ih + 64] = value[64:]

    for n in range(15):
        m_copy(None, n).wait_recv()

    for n in range(15):
        g_copy(n).wait_send()

    @pl.loop(0, SLOTS)
    def _(slot):
        for n in range(15):
            d_copy(slot, n).wait_send()
        for hop in range(4):
            ahead_copy(slot, hop).wait_send()
        for hop in range(3):
            behind_copy(slot, hop).wait_send()
        for n in range(8):
            partner_copy(slot, n).wait_send()

    @pl.loop(0, SLOTS - 1)
    def _(slot):
        for n in range(15):
            m_copy(slot, n).wait_send()

    for n in range(15):
        m_copy(None, n).wait_send()


def finish(acc_ref, m_last, tail_hi, tail_lo, out_hbm, o_buf, o_sem):
    def out_copy(group, half):
        rows = pl.ds(half * 64 + group * 4, 4)
        return pltpu.make_async_copy(o_buf.at[rows], out_hbm.at[rows], o_sem.at[group, half])

    @pl.loop(0, 8)
    def _(pair):
        for u in range(2):
            group = pair * 2 + u
            first = group * 4
            part = jnp.concatenate([m_last[:, first + v, :] for v in range(4)], axis=0)
            high, low = split(part.T)
            value = jnp.dot(
                jnp.concatenate([high, low], axis=1), tail_hi[...], preferred_element_type=F32
            ) + jnp.dot(high, tail_lo[...], preferred_element_type=F32)
            for v in range(4):
                for half in range(2):
                    at = half * 64 + first + v
                    o_buf[at] = acc_ref[at] + value[half * 64:(half + 1) * 64, v * 128:(v + 1) * 128]
            for half in range(2):
                out_copy(group, half).start()

    @pl.loop(0, 16)
    def _(group):
        for half in range(2):
            out_copy(group, half).wait()


def local(recorded, panels):
    tables, tails = jax.tree.map(jnp.asarray, lookup_tables())
    dma = pltpu.SemaphoreType.DMA
    whole = pl.BlockSpec(memory_space=pltpu.VMEM)
    acc, last = pl.pallas_call(
        kernel,
        out_shape=(pltpu.VMEM((128, 64, NT), F32), pltpu.VMEM((32, PITCH, 128), F32)),
        in_specs=[
            pl.BlockSpec(memory_space=pl.ANY),
            pl.BlockSpec(memory_space=pl.ANY),
            whole, whole, whole, whole,
        ],
        out_specs=(whole, whole),
        scratch_shapes=[
            pltpu.VMEM((128, 64, NT), F32),
            pltpu.VMEM((16, 64, NT), F32),
            pltpu.VMEM((1024, 128), F32),
            pltpu.VMEM((16, 64, 128), F32),
            pltpu.VMEM((SLOTS, 16, 2, 2, 16, 512), F32),
            pltpu.VMEM((128, PITCH, 128), F32),
            pltpu.VMEM((SLOTS, 16, 2, 64, 128), F32),
            pltpu.VMEM((2, 256, 512), BF16),
            pltpu.VMEM((2, 256, 512), BF16),
            pltpu.VMEM((2, 512, 512), BF16),
            pltpu.VMEM((2, 512, 512), BF16),
            pltpu.VMEM((SLOTS, 16, 2, 64, 128), F32),
            pltpu.VMEM((SLOTS - 1, 32, PITCH, 128), F32),
            dma((4, 2)), dma,
            dma((15,)), dma((15,)),
            dma((SLOTS, 15)), dma((SLOTS, 15)),
            dma((SLOTS, 15)), dma((SLOTS, 15)),
            dma((SLOTS, 4)), dma((SLOTS, 4)),
            dma((SLOTS, 3)), dma((SLOTS, 3)),
            dma((SLOTS, 8)), dma((SLOTS, 8)),
        ],
        compiler_params=pltpu.CompilerParams(
            collective_id=0, has_side_effects=True, vmem_limit_bytes=52 * 1024 * 1024
        ),
        name="convolve",
    )(recorded, panels, *tables)
    return pl.pallas_call(
        finish,
        out_shape=jax.ShapeDtypeStruct((128, 64, NT), F32),
        in_specs=[whole, whole, whole, whole],
        out_specs=pl.BlockSpec(memory_space=pl.ANY),
        scratch_shapes=[pltpu.VMEM((128, 64, NT), F32), dma((16, 2))],
        compiler_params=pltpu.CompilerParams(vmem_limit_bytes=16 * 1024 * 1024),
        name="finish",
    )(acc, last, *tails)


def solution(mesh):
    return jax.shard_map(
        local,
        mesh=mesh,
        in_specs=(P("src", "freq", None), P("src", "freq", None)),
        out_specs=P("src", "freq", None),
        check_vma=False,
    )
```

```python
import functools

import jax
import jax.numpy as jnp
import numpy as np
from jax import lax
from jax.experimental import pallas as pl
from jax.experimental.pallas import tpu as pltpu
from jax.sharding import PartitionSpec as P

NT = 128
NF = 64
SLOTS = 4
PITCH = 72
MESH = pl.DeviceIdType.MESH
F32 = jnp.float32
BF16 = jnp.bfloat16

PLANE = [
    (1, 0), (0, 1), (3, 0), (0, 3), (1, 2), (2, 1), (3, 2), (2, 3),
    (1, 1), (3, 3), (2, 2), (1, 3), (3, 1), (2, 0), (0, 2),
]


def lookup_tables():
    phase = np.arange(NF)[:, None] * np.arange(NT)[None, :] % NT
    angle = 2.0 * np.pi / NT * phase
    forward = np.stack([np.cos(angle), -np.sin(angle)], axis=1)
    weight = np.where(np.arange(NF) == 0, 1.0, 2.0) / NT
    inverse = forward * weight[:, None, None]
    by_owner = forward.reshape(2 * NF, NT)
    forward, inverse = (
        table.reshape(16, SLOTS, 2, NT).transpose(1, 0, 2, 3).reshape(2 * NF, NT) for table in (forward, inverse)
    )
    tables = np.stack([part for table in (by_owner, forward, inverse) for part in split_table(table)])
    tail_hi, tail_lo = (np.kron(np.eye(4), part[96:].astype(np.float32)).astype(BF16) for part in tables[4:])
    return tables, (np.concatenate([tail_hi, tail_hi]), tail_lo)


def split_table(table):
    high = table.astype(np.float32).astype(BF16)
    low = (table - high.astype(np.float64)).astype(np.float32).astype(BF16)
    return high, low


def split(value):
    high = value.astype(BF16)
    return high, (value - high.astype(F32)).astype(BF16)


def halves(first, second):
    lane = lax.broadcasted_iota(jnp.int32, first.shape, first.ndim - 1)
    low = jnp.where(lane < 64, first, pltpu.roll(second, 64, axis=first.ndim - 1))
    high = jnp.where(lane < 64, pltpu.roll(first, 64, axis=first.ndim - 1), second)
    return low, high


def kernel(
    rec_hbm, pan_hbm, table_hbm, acc_ref, m_last,
    tables, x_buf, p_buf, g_send, g_recv, g_all, d_send, d_recv, d_hi, d_lo, g_hi, g_lo, m_send, m_recv,
    t_sem, x_sem, p_sem, gs_sem, gr_sem, ds_sem, dr_sem, ms_sem, mr_sem,
    fs_sem, fr_sem, bs_sem, br_sem, cs_sem, cr_sem,
):
    own_o = lax.axis_index("freq")
    src = lax.axis_index("src")
    own_xhi = src // 16
    zc = lax.rem(src, 16)
    z = zc // 2
    core = lax.rem(zc, 2)
    x = own_xhi * 2 + own_o // 4
    y = lax.rem(own_o, 4)
    own_q = own_xhi * 8 + own_o

    def plane(offset):
        px = lax.rem(x + offset[0], 4)
        py = lax.rem(y + offset[1], 4)
        o = lax.rem(px, 2) * 4 + py
        return o, px // 2

    def plane_id(offset):
        o, xhi = plane(offset)
        return (o, xhi * 16 + zc)

    step = 1 - 2 * core
    z_ahead = lax.rem(z + step + 8, 8)
    z_behind = lax.rem(z - step + 8, 8)
    ahead_id = (own_o, own_xhi * 16 + z_ahead * 2 + core)
    behind_id = (own_o, own_xhi * 16 + z_behind * 2 + core)
    partner_id = (own_o, own_xhi * 16 + z * 2 + 1 - core)

    pan_copy = pltpu.make_async_copy(pan_hbm, p_buf, p_sem)
    pan_copy.start()
    table_copy = pltpu.make_async_copy(table_hbm, tables, t_sem)
    table_copy.start()

    def rec_copy(chunk, half):
        rows = pl.ds(half * 64 + chunk * 16, 16)
        return pltpu.make_async_copy(rec_hbm.at[rows], x_buf.at[rows], x_sem.at[chunk, half])

    for chunk in range(4):
        for half in range(2):
            rec_copy(chunk, half).start()

    barrier = pltpu.get_barrier_semaphore()
    others = [plane_id(offset) for offset in PLANE] + [ahead_id, behind_id, partner_id]
    for other in others:
        pl.semaphore_signal(barrier, inc=1, device_id=other, device_id_type=MESH)

    nt = (((1,), (1,)), ((), ()))

    def forward(table, freqs, rows):
        high, low = split(rows)
        fwd_hi, fwd_lo = tables[table, freqs, :], tables[table + 1, freqs, :]
        return (
            lax.dot_general(fwd_hi, high, nt, preferred_element_type=F32)
            + lax.dot_general(fwd_hi, low, nt, preferred_element_type=F32)
            + lax.dot_general(fwd_lo, high, nt, preferred_element_type=F32)
        )

    pan_copy.wait()
    table_copy.wait()
    for kp in range(0, 8, 2):
        rows = jnp.concatenate([p_buf[kp], p_buf[kp + 8], p_buf[kp + 1], p_buf[kp + 9]], axis=0)
        hat = forward(0, slice(0, 128), rows)
        g_send[pl.ds(kp, 128, stride=8), :] = hat[:, :128]
        g_send[pl.ds(kp + 1, 128, stride=8), :] = hat[:, 128:]

    pl.semaphore_wait(barrier, len(others))

    def g_copy(n):
        o, xhi = plane(PLANE[n])
        return pltpu.make_async_remote_copy(
            src_ref=g_send.at[pl.ds((xhi * 8 + o) * 64, 64)],
            dst_ref=g_recv.at[own_q],
            send_sem=gs_sem.at[n], recv_sem=gr_sem.at[n],
            device_id=plane_id(PLANE[n]), device_id_type=MESH,
        )

    for n in range(15):
        g_copy(n).start()
    g_recv[own_q] = g_send[pl.ds(own_q * 64, 64), :]

    def d_copy(slot, n):
        o, xhi = plane(PLANE[n])
        return pltpu.make_async_remote_copy(
            src_ref=d_send.at[pl.ds(slot * 32 + (xhi * 8 + o) * 2, 2), pl.ds(0, 64)],
            dst_ref=d_recv.at[slot, own_q],
            send_sem=ds_sem.at[slot, n], recv_sem=dr_sem.at[slot, n],
            device_id=plane_id(PLANE[n]), device_id_type=MESH,
        )

    def spectra(start, count, ih):
        rows = jnp.concatenate([x_buf[ih], x_buf[ih + 64], x_buf[ih + 1], x_buf[ih + 65]], axis=0)
        freqs = slice(start, start + count)
        hat = forward(2, freqs, rows)
        d_send[freqs, ih, :] = hat[:, :128]
        d_send[freqs, ih + 1, :] = hat[:, 128:]

    def d_start(slot):
        for n in range(15):
            d_copy(slot, n).start()
        d_recv[slot, own_q] = d_send[pl.ds(slot * 32 + own_q * 2, 2), 0:64, :]

    for chunk in range(4):
        for half in range(2):
            rec_copy(chunk, half).wait()

        @pl.loop(0, 4)
        def _(quad):
            for u in range(2):
                spectra(0, 32, chunk * 16 + quad * 4 + u * 2)

    d_start(0)

    @pl.loop(0, 32)
    def _(pair):
        spectra(32, 96, pair * 2)

    @pl.loop(1, SLOTS)
    def _(slot):
        d_start(slot)

    for n in range(15):
        g_copy(n).wait_recv()

    @pl.loop(0, SLOTS)
    def _(slot):
        for c in range(2):
            rows = pl.ds((slot * 2 + c) * 8, 8)
            for xhi in range(2):
                for pair in range(4):
                    low, high = halves(g_recv[xhi * 8 + 2 * pair, rows, :], g_recv[xhi * 8 + 2 * pair + 1, rows, :])
                    g_all[slot, zc, c, xhi, 0:8, pair * 128:(pair + 1) * 128] = low
                    g_all[slot, zc, c, xhi, 8:16, pair * 128:(pair + 1) * 128] = high

    def block(hop, way):
        return lax.rem(z - way * hop * step + 32, 8) * 2 + core

    def ahead_copy(slot, hop):
        ref = g_all.at[slot, block(hop, 1)]
        return pltpu.make_async_remote_copy(
            src_ref=ref, dst_ref=ref, send_sem=fs_sem.at[slot, hop], recv_sem=fr_sem.at[slot, hop],
            device_id=ahead_id, device_id_type=MESH,
        )

    def behind_copy(slot, hop):
        ref = g_all.at[slot, block(hop, -1)]
        return pltpu.make_async_remote_copy(
            src_ref=ref, dst_ref=ref, send_sem=bs_sem.at[slot, hop], recv_sem=br_sem.at[slot, hop],
            device_id=behind_id, device_id_type=MESH,
        )

    def partner_copy(slot, n):
        ref = g_all.at[slot, block(n, 1) if n < 5 else block(n - 4, -1)]
        return pltpu.make_async_remote_copy(
            src_ref=ref, dst_ref=ref, send_sem=cs_sem.at[slot, n], recv_sem=cr_sem.at[slot, n],
            device_id=partner_id, device_id_type=MESH,
        )

    def first(slot):
        ahead_copy(slot, 0).start()
        behind_copy(slot, 0).start()
        partner_copy(slot, 0).start()

    def pass_on(hop, slot):
        ahead_copy(slot, hop).wait_recv()
        if hop < 3:
            ahead_copy(slot, hop + 1).start()
        partner_copy(slot, hop + 1).start()
        if hop < 3:
            behind_copy(slot, hop).wait_recv()
            if hop < 2:
                behind_copy(slot, hop + 1).start()
            partner_copy(slot, hop + 5).start()

    first(0)
    first(1)
    pass_on(0, 0)
    first(2)
    pass_on(1, 0)
    pass_on(0, 1)
    first(3)
    pass_on(2, 0)
    pass_on(1, 1)
    pass_on(0, 2)

    def m_copy(slot, n):
        o, xhi = plane(PLANE[n])
        if slot is None:
            slot, dst = SLOTS - 1, m_last
        else:
            dst = m_recv.at[slot]
        return pltpu.make_async_remote_copy(
            src_ref=m_send.at[slot, xhi * 8 + o],
            dst_ref=dst.at[pl.ds(own_q * 2, 2), pl.ds(0, 64)],
            send_sem=ms_sem.at[slot, n], recv_sem=mr_sem.at[slot, n],
            device_id=plane_id(PLANE[n]), device_id_type=MESH,
        )

    def dot(left, right):
        return jnp.dot(left, right, preferred_element_type=F32)

    def predict(slot):
        for n in range(8):
            partner_copy(slot, n).wait_recv()

        @pl.loop(0, 16)
        def _(b):
            for c in range(2):
                for xhi in range(2):
                    high, low = split(g_all[slot, b, c, xhi])
                    rows = pl.ds(xhi * 256 + b * 16, 16)
                    g_hi[c, rows, :] = high
                    g_lo[c, rows, :] = low

        for n in range(15):
            d_copy(slot, n).wait_recv()

        for xhi in range(2):
            for pair in range(4):
                for c in range(2):
                    top, bottom = halves(
                        d_recv[slot, xhi * 8 + 2 * pair, c], d_recv[slot, xhi * 8 + 2 * pair + 1, c]
                    )
                    for at, part in ((0, top), (64, bottom)):
                        high, low = split(part)
                        d_hi[c, xhi * 128 + at:xhi * 128 + at + 64, pair * 128:(pair + 1) * 128] = high
                        d_lo[c, xhi * 128 + at:xhi * 128 + at + 64, pair * 128:(pair + 1) * 128] = low

        @pl.loop(0, 2)
        def _(xhi):
            rows = pl.ds(xhi * 128, 128)
            for tile in range(2):
                cols = slice(tile * 256, (tile + 1) * 256)

                def product(a, b):
                    return (
                        dot(d_hi[a, rows, :], g_hi[b, :, cols])
                        + dot(d_hi[a, rows, :], g_lo[b, :, cols])
                        + dot(d_lo[a, rows, :], g_hi[b, :, cols])
                    )

                real = product(0, 0) - product(1, 1)
                imag = product(0, 1) + product(1, 0)
                for c, value in ((0, real), (1, imag)):
                    for lanes in range(2):
                        part = value[:, lanes * 128:(lanes + 1) * 128]
                        even, odd = halves(part[:64], part[64:])
                        o = tile * 4 + lanes * 2
                        m_send[slot, xhi * 8 + o, c] = even
                        m_send[slot, xhi * 8 + o + 1, c] = odd

    @pl.loop(0, SLOTS - 1)
    def _(slot):
        pass_on(3, slot)
        pass_on(2, slot + 1)

        @pl.when(slot < 2)
        def _():
            pass_on(1, slot + 2)

        @pl.when(slot < 1)
        def _():
            pass_on(0, slot + 3)

        predict(slot)
        for n in range(15):
            m_copy(slot, n).start()
        m_recv[slot, pl.ds(own_q * 2, 2), 0:64, :] = m_send[slot, own_q]

    pass_on(3, SLOTS - 1)
    predict(SLOTS - 1)
    for n in range(15):
        m_copy(None, n).start()
    m_last[pl.ds(own_q * 2, 2), 0:64, :] = m_send[SLOTS - 1, own_q]

    def arrive(slot):
        for n in range(15):
            m_copy(slot, n).wait_recv()

    def back(first, slots, ih):
        part = jnp.concatenate([m_recv[slot, :, ih, :] for slot in range(first, first + slots)], axis=0)
        high, low = split(part.T)
        freqs = slice(first * 32, (first + slots) * 32)
        inv_hi, inv_lo = tables[4, freqs, :], tables[5, freqs, :]
        return dot(high, inv_hi) + dot(low, inv_hi) + dot(high, inv_lo)

    arrive(0)
    arrive(1)

    @pl.loop(0, 32)
    def _(pair):
        for u in range(2):
            ih = pair * 2 + u
            value = back(0, 2, ih)
            acc_ref[ih] = value[:64]
            acc_ref[ih + 64] = value[64:]

    arrive(2)

    @pl.loop(0, 32)
    def _(pair):
        for u in range(2):
            ih = pair * 2 + u
            value = back(2, 1, ih)
            acc_ref[ih] += value[:64]
            acc_ref[ih + 64] += value[64:]

    for n in range(15):
        m_copy(None, n).wait_recv()

    for n in range(15):
        g_copy(n).wait_send()

    @pl.loop(0, SLOTS)
    def _(slot):
        for n in range(15):
            d_copy(slot, n).wait_send()
        for hop in range(4):
            ahead_copy(slot, hop).wait_send()
        for hop in range(3):
            behind_copy(slot, hop).wait_send()
        for n in range(8):
            partner_copy(slot, n).wait_send()

    @pl.loop(0, SLOTS - 1)
    def _(slot):
        for n in range(15):
            m_copy(slot, n).wait_send()

    for n in range(15):
        m_copy(None, n).wait_send()


def finish(acc_ref, m_last, tail_hi, tail_lo, out_hbm, o_buf, o_sem):
    def out_copy(group, half):
        rows = pl.ds(half * 64 + group * 4, 4)
        return pltpu.make_async_copy(o_buf.at[rows], out_hbm.at[rows], o_sem.at[group, half])

    @pl.loop(0, 8)
    def _(pair):
        for u in range(2):
            group = pair * 2 + u
            first = group * 4
            part = jnp.concatenate([m_last[:, first + v, :] for v in range(4)], axis=0)
            high, low = split(part.T)
            value = jnp.dot(
                jnp.concatenate([high, low], axis=1), tail_hi[...], preferred_element_type=F32
            ) + jnp.dot(high, tail_lo[...], preferred_element_type=F32)
            for v in range(4):
                for half in range(2):
                    at = half * 64 + first + v
                    o_buf[at] = acc_ref[at] + value[half * 64:(half + 1) * 64, v * 128:(v + 1) * 128]
            for half in range(2):
                out_copy(group, half).start()

    @pl.loop(0, 16)
    def _(group):
        for half in range(2):
            out_copy(group, half).wait()


def local(recorded, panels):
    tables, tails = jax.tree.map(jnp.asarray, lookup_tables())
    dma = pltpu.SemaphoreType.DMA
    whole = pl.BlockSpec(memory_space=pltpu.VMEM)
    acc, last = pl.pallas_call(
        kernel,
        out_shape=(pltpu.VMEM((128, 64, NT), F32), pltpu.VMEM((32, PITCH, 128), F32)),
        in_specs=[
            pl.BlockSpec(memory_space=pl.ANY),
            pl.BlockSpec(memory_space=pl.ANY),
            pl.BlockSpec(memory_space=pl.ANY),
        ],
        out_specs=(whole, whole),
        scratch_shapes=[
            pltpu.VMEM((6, 128, NT), BF16),
            pltpu.VMEM((128, 64, NT), F32),
            pltpu.VMEM((16, 64, NT), F32),
            pltpu.VMEM((1024, 128), F32),
            pltpu.VMEM((16, 64, 128), F32),
            pltpu.VMEM((SLOTS, 16, 2, 2, 16, 512), F32),
            pltpu.VMEM((128, PITCH, 128), F32),
            pltpu.VMEM((SLOTS, 16, 2, 64, 128), F32),
            pltpu.VMEM((2, 256, 512), BF16),
            pltpu.VMEM((2, 256, 512), BF16),
            pltpu.VMEM((2, 512, 512), BF16),
            pltpu.VMEM((2, 512, 512), BF16),
            pltpu.VMEM((SLOTS, 16, 2, 64, 128), F32),
            pltpu.VMEM((SLOTS - 1, 32, PITCH, 128), F32),
            dma, dma((4, 2)), dma,
            dma((15,)), dma((15,)),
            dma((SLOTS, 15)), dma((SLOTS, 15)),
            dma((SLOTS, 15)), dma((SLOTS, 15)),
            dma((SLOTS, 4)), dma((SLOTS, 4)),
            dma((SLOTS, 3)), dma((SLOTS, 3)),
            dma((SLOTS, 8)), dma((SLOTS, 8)),
        ],
        compiler_params=pltpu.CompilerParams(
            collective_id=0, has_side_effects=True, vmem_limit_bytes=52 * 1024 * 1024
        ),
        name="convolve",
    )(recorded, panels, tables)
    return pl.pallas_call(
        finish,
        out_shape=jax.ShapeDtypeStruct((128, 64, NT), F32),
        in_specs=[whole, whole, whole, whole],
        out_specs=pl.BlockSpec(memory_space=pl.ANY),
        scratch_shapes=[pltpu.VMEM((128, 64, NT), F32), dma((16, 2))],
        compiler_params=pltpu.CompilerParams(vmem_limit_bytes=16 * 1024 * 1024),
        name="finish",
    )(acc, last, *tails)


def solution(mesh):
    return jax.shard_map(
        local,
        mesh=mesh,
        in_specs=(P("src", "freq", None), P("src", "freq", None)),
        out_specs=P("src", "freq", None),
        check_vma=False,
    )
```

```python
import functools

import jax
import jax.numpy as jnp
import numpy as np
from jax import lax
from jax.experimental import pallas as pl
from jax.experimental.pallas import tpu as pltpu
from jax.sharding import PartitionSpec as P

NT = 128
NF = 64
SLOTS = 4
PITCH = 72
GROUPS = 4
MESH = pl.DeviceIdType.MESH
F32 = jnp.float32
BF16 = jnp.bfloat16

PLANE = [
    (1, 0), (0, 1), (3, 0), (0, 3), (1, 2), (2, 1), (3, 2), (2, 3),
    (1, 1), (3, 3), (2, 2), (1, 3), (3, 1), (2, 0), (0, 2),
]


def lookup_tables():
    phase = np.arange(NF)[:, None] * np.arange(NT)[None, :] % NT
    angle = 2.0 * np.pi / NT * phase
    forward = np.stack([np.cos(angle), -np.sin(angle)], axis=1)
    weight = np.where(np.arange(NF) == 0, 1.0, 2.0) / NT
    inverse = forward * weight[:, None, None]
    by_owner = forward.reshape(2 * NF, NT)
    forward, inverse = (
        table.reshape(16, SLOTS, 2, NT).transpose(1, 0, 2, 3).reshape(2 * NF, NT) for table in (forward, inverse)
    )
    tables = np.stack([part for table in (by_owner, forward, inverse) for part in split_table(table)])
    tail_hi, tail_lo = (np.kron(np.eye(4), part[96:].astype(np.float32)).astype(BF16) for part in tables[4:])
    return tables, (np.concatenate([tail_hi, tail_hi]), tail_lo)


def split_table(table):
    high = table.astype(np.float32).astype(BF16)
    low = (table - high.astype(np.float64)).astype(np.float32).astype(BF16)
    return high, low


def split(value):
    high = value.astype(BF16)
    return high, (value - high.astype(F32)).astype(BF16)


def halves(first, second):
    lane = lax.broadcasted_iota(jnp.int32, first.shape, first.ndim - 1)
    low = jnp.where(lane < 64, first, pltpu.roll(second, 64, axis=first.ndim - 1))
    high = jnp.where(lane < 64, pltpu.roll(first, 64, axis=first.ndim - 1), second)
    return low, high


def kernel(
    rec_hbm, pan_hbm, table_hbm, acc_ref, m_last,
    tables, x_buf, p_buf, g_send, g_recv, g_all, d_send, d_recv, d_hi, d_lo, g_hi, g_lo, m_send, m_recv,
    t_sem, x_sem, p_sem, gs_sem, gr_sem, ds_sem, dr_sem, ms_sem, mr_sem,
    fs_sem, fr_sem, bs_sem, br_sem, cs_sem, cr_sem,
):
    own_o = lax.axis_index("freq")
    src = lax.axis_index("src")
    own_xhi = src // 16
    zc = lax.rem(src, 16)
    z = zc // 2
    core = lax.rem(zc, 2)
    x = own_xhi * 2 + own_o // 4
    y = lax.rem(own_o, 4)
    own_q = own_xhi * 8 + own_o

    def plane(offset):
        px = lax.rem(x + offset[0], 4)
        py = lax.rem(y + offset[1], 4)
        o = lax.rem(px, 2) * 4 + py
        return o, px // 2

    def plane_id(offset):
        o, xhi = plane(offset)
        return (o, xhi * 16 + zc)

    step = 1 - 2 * core
    z_ahead = lax.rem(z + step + 8, 8)
    z_behind = lax.rem(z - step + 8, 8)
    ahead_id = (own_o, own_xhi * 16 + z_ahead * 2 + core)
    behind_id = (own_o, own_xhi * 16 + z_behind * 2 + core)
    partner_id = (own_o, own_xhi * 16 + z * 2 + 1 - core)

    pan_copy = pltpu.make_async_copy(pan_hbm, p_buf, p_sem)
    pan_copy.start()
    table_copy = pltpu.make_async_copy(table_hbm, tables, t_sem)
    table_copy.start()

    def rec_copy(chunk, half):
        rows = pl.ds(half * 64 + chunk * 16, 16)
        return pltpu.make_async_copy(rec_hbm.at[rows], x_buf.at[rows], x_sem.at[chunk, half])

    for chunk in range(4):
        for half in range(2):
            rec_copy(chunk, half).start()

    barrier = pltpu.get_barrier_semaphore()
    others = [plane_id(offset) for offset in PLANE] + [ahead_id, behind_id, partner_id]
    for other in others:
        pl.semaphore_signal(barrier, inc=1, device_id=other, device_id_type=MESH)

    nt = (((1,), (1,)), ((), ()))

    def forward(table, freqs, rows):
        high, low = split(rows)
        fwd_hi, fwd_lo = tables[table, freqs, :], tables[table + 1, freqs, :]
        return (
            lax.dot_general(fwd_hi, high, nt, preferred_element_type=F32)
            + lax.dot_general(fwd_hi, low, nt, preferred_element_type=F32)
            + lax.dot_general(fwd_lo, high, nt, preferred_element_type=F32)
        )

    pan_copy.wait()
    table_copy.wait()
    for kp in range(0, 8, 2):
        rows = jnp.concatenate([p_buf[kp], p_buf[kp + 8], p_buf[kp + 1], p_buf[kp + 9]], axis=0)
        hat = forward(0, slice(0, 128), rows)
        g_send[kp] = hat[:, :128]
        g_send[kp + 1] = hat[:, 128:]

    pl.semaphore_wait(barrier, len(others))

    def g_copy(n):
        o, xhi = plane(PLANE[n])
        return pltpu.make_async_remote_copy(
            src_ref=g_send.at[:, pl.ds((xhi * 8 + o) * 8, 8)],
            dst_ref=g_recv.at[own_q],
            send_sem=gs_sem.at[n], recv_sem=gr_sem.at[n],
            device_id=plane_id(PLANE[n]), device_id_type=MESH,
        )

    for n in range(15):
        g_copy(n).start()
    g_recv[own_q] = g_send[:, pl.ds(own_q * 8, 8), :]

    def d_copy(slot, n):
        o, xhi = plane(PLANE[n])
        return pltpu.make_async_remote_copy(
            src_ref=d_send.at[pl.ds(slot * 32 + (xhi * 8 + o) * 2, 2), pl.ds(0, 64)],
            dst_ref=d_recv.at[slot, own_q],
            send_sem=ds_sem.at[slot, n], recv_sem=dr_sem.at[slot, n],
            device_id=plane_id(PLANE[n]), device_id_type=MESH,
        )

    def spectra(start, count, ih):
        rows = jnp.concatenate([x_buf[ih], x_buf[ih + 64], x_buf[ih + 1], x_buf[ih + 65]], axis=0)
        freqs = slice(start, start + count)
        hat = forward(2, freqs, rows)
        d_send[freqs, ih, :] = hat[:, :128]
        d_send[freqs, ih + 1, :] = hat[:, 128:]

    def d_start(slot):
        for n in range(15):
            d_copy(slot, n).start()
        d_recv[slot, own_q] = d_send[pl.ds(slot * 32 + own_q * 2, 2), 0:64, :]

    for chunk in range(4):
        for half in range(2):
            rec_copy(chunk, half).wait()

        @pl.loop(0, 4)
        def _(quad):
            for u in range(2):
                spectra(0, 32, chunk * 16 + quad * 4 + u * 2)

    d_start(0)

    @pl.loop(0, 32)
    def _(pair):
        spectra(32, 96, pair * 2)

    @pl.loop(1, SLOTS)
    def _(slot):
        d_start(slot)

    for n in range(15):
        g_copy(n).wait_recv()

    @pl.loop(0, SLOTS)
    def _(slot):
        for c in range(2):
            row = slot * 2 + c
            for xhi in range(2):
                for pair in range(4):
                    low, high = halves(
                        g_recv[xhi * 8 + 2 * pair, :, row, :], g_recv[xhi * 8 + 2 * pair + 1, :, row, :]
                    )
                    g_all[slot, zc, c, xhi, 0:8, pair * 128:(pair + 1) * 128] = low
                    g_all[slot, zc, c, xhi, 8:16, pair * 128:(pair + 1) * 128] = high

    def block(hop, way):
        return lax.rem(z - way * hop * step + 32, 8) * 2 + core

    def ahead_copy(slot, hop):
        ref = g_all.at[slot, block(hop, 1)]
        return pltpu.make_async_remote_copy(
            src_ref=ref, dst_ref=ref, send_sem=fs_sem.at[slot, hop], recv_sem=fr_sem.at[slot, hop],
            device_id=ahead_id, device_id_type=MESH,
        )

    def behind_copy(slot, hop):
        ref = g_all.at[slot, block(hop, -1)]
        return pltpu.make_async_remote_copy(
            src_ref=ref, dst_ref=ref, send_sem=bs_sem.at[slot, hop], recv_sem=br_sem.at[slot, hop],
            device_id=behind_id, device_id_type=MESH,
        )

    def partner_copy(slot, n):
        ref = g_all.at[slot, block(n, 1) if n < 5 else block(n - 4, -1)]
        return pltpu.make_async_remote_copy(
            src_ref=ref, dst_ref=ref, send_sem=cs_sem.at[slot, n], recv_sem=cr_sem.at[slot, n],
            device_id=partner_id, device_id_type=MESH,
        )

    def first(slot):
        ahead_copy(slot, 0).start()
        behind_copy(slot, 0).start()
        partner_copy(slot, 0).start()

    def pass_on(hop, slot):
        ahead_copy(slot, hop).wait_recv()
        if hop < 3:
            ahead_copy(slot, hop + 1).start()
        partner_copy(slot, hop + 1).start()
        if hop < 3:
            behind_copy(slot, hop).wait_recv()
            if hop < 2:
                behind_copy(slot, hop + 1).start()
            partner_copy(slot, hop + 5).start()

    first(0)
    first(1)
    pass_on(0, 0)
    first(2)
    pass_on(1, 0)
    pass_on(0, 1)
    first(3)
    pass_on(2, 0)
    pass_on(1, 1)
    pass_on(0, 2)

    def m_copy(slot, n):
        o, xhi = plane(PLANE[n])
        if slot is None:
            slot, dst = SLOTS - 1, m_last
        else:
            dst = m_recv.at[slot]
        return pltpu.make_async_remote_copy(
            src_ref=m_send.at[slot, xhi * 8 + o],
            dst_ref=dst.at[pl.ds(own_q * 2, 2), pl.ds(0, 64)],
            send_sem=ms_sem.at[slot, n], recv_sem=mr_sem.at[slot, n],
            device_id=plane_id(PLANE[n]), device_id_type=MESH,
        )

    def dot(left, right):
        return jnp.dot(left, right, preferred_element_type=F32)

    def predict(slot):
        for n in range(8):
            partner_copy(slot, n).wait_recv()

        @pl.loop(0, 16)
        def _(b):
            for c in range(2):
                for xhi in range(2):
                    high, low = split(g_all[slot, b, c, xhi])
                    rows = pl.ds(xhi * 256 + b * 16, 16)
                    g_hi[c, rows, :] = high
                    g_lo[c, rows, :] = low

        for n in range(15):
            d_copy(slot, n).wait_recv()

        for xhi in range(2):
            for pair in range(4):
                for c in range(2):
                    top, bottom = halves(
                        d_recv[slot, xhi * 8 + 2 * pair, c], d_recv[slot, xhi * 8 + 2 * pair + 1, c]
                    )
                    for at, part in ((0, top), (64, bottom)):
                        high, low = split(part)
                        d_hi[c, xhi * 128 + at:xhi * 128 + at + 64, pair * 128:(pair + 1) * 128] = high
                        d_lo[c, xhi * 128 + at:xhi * 128 + at + 64, pair * 128:(pair + 1) * 128] = low

        @pl.loop(0, 2)
        def _(xhi):
            rows = pl.ds(xhi * 128, 128)
            for tile in range(2):
                cols = slice(tile * 256, (tile + 1) * 256)

                def product(a, b):
                    return (
                        dot(d_hi[a, rows, :], g_hi[b, :, cols])
                        + dot(d_hi[a, rows, :], g_lo[b, :, cols])
                        + dot(d_lo[a, rows, :], g_hi[b, :, cols])
                    )

                real = product(0, 0) - product(1, 1)
                imag = product(0, 1) + product(1, 0)
                for c, value in ((0, real), (1, imag)):
                    for lanes in range(2):
                        part = value[:, lanes * 128:(lanes + 1) * 128]
                        even, odd = halves(part[:64], part[64:])
                        o = tile * 4 + lanes * 2
                        m_send[slot, xhi * 8 + o, c] = even
                        m_send[slot, xhi * 8 + o + 1, c] = odd

    @pl.loop(0, SLOTS - 1)
    def _(slot):
        pass_on(3, slot)
        pass_on(2, slot + 1)

        @pl.when(slot < 2)
        def _():
            pass_on(1, slot + 2)

        @pl.when(slot < 1)
        def _():
            pass_on(0, slot + 3)

        predict(slot)
        for n in range(15):
            m_copy(slot, n).start()
        m_recv[slot, pl.ds(own_q * 2, 2), 0:64, :] = m_send[slot, own_q]

    pass_on(3, SLOTS - 1)
    predict(SLOTS - 1)
    for n in range(15):
        m_copy(None, n).start()
    m_last[pl.ds(own_q * 2, 2), 0:64, :] = m_send[SLOTS - 1, own_q]

    def arrive(slot):
        for n in range(15):
            m_copy(slot, n).wait_recv()

    def back(first, slots, ih):
        part = jnp.concatenate([m_recv[slot, :, ih, :] for slot in range(first, first + slots)], axis=0)
        high, low = split(part.T)
        freqs = slice(first * 32, (first + slots) * 32)
        inv_hi, inv_lo = tables[4, freqs, :], tables[5, freqs, :]
        return dot(high, inv_hi) + dot(low, inv_hi) + dot(high, inv_lo)

    arrive(0)
    arrive(1)

    @pl.loop(0, 32)
    def _(pair):
        for u in range(2):
            ih = pair * 2 + u
            value = back(0, 2, ih)
            acc_ref[ih] = value[:64]
            acc_ref[ih + 64] = value[64:]

    arrive(2)

    @pl.loop(0, 32)
    def _(pair):
        for u in range(2):
            ih = pair * 2 + u
            value = back(2, 1, ih)
            acc_ref[ih] += value[:64]
            acc_ref[ih + 64] += value[64:]

    for n in range(15):
        m_copy(None, n).wait_recv()

    for n in range(15):
        g_copy(n).wait_send()

    @pl.loop(0, SLOTS)
    def _(slot):
        for n in range(15):
            d_copy(slot, n).wait_send()
        for hop in range(4):
            ahead_copy(slot, hop).wait_send()
        for hop in range(3):
            behind_copy(slot, hop).wait_send()
        for n in range(8):
            partner_copy(slot, n).wait_send()

    @pl.loop(0, SLOTS - 1)
    def _(slot):
        for n in range(15):
            m_copy(slot, n).wait_send()

    for n in range(15):
        m_copy(None, n).wait_send()


def finish(acc_ref, m_last, tail_hi, tail_lo, out_hbm, o_buf, o_sem):
    def out_copy(group, half):
        rows = pl.ds(half * 64 + group * 4, 4)
        return pltpu.make_async_copy(o_buf.at[rows], out_hbm.at[rows], o_sem.at[group, half])

    @pl.loop(0, 16 // GROUPS)
    def _(step):
        parts = []
        for u in range(GROUPS):
            first = (step * GROUPS + u) * 4
            part = jnp.concatenate([m_last[pl.ds(first + v, 32, stride=PITCH), :] for v in range(4)], axis=0)
            parts.append(split(part.T))
        both = jnp.concatenate([jnp.concatenate(part, axis=1) for part in parts], axis=0)
        highs = jnp.concatenate([high for high, _ in parts], axis=0)
        value = jnp.dot(both, tail_hi[...], preferred_element_type=F32) + jnp.dot(
            highs, tail_lo[...], preferred_element_type=F32
        )
        for u in range(GROUPS):
            group = step * GROUPS + u
            for v in range(4):
                for half in range(2):
                    at = half * 64 + group * 4 + v
                    rows = slice(u * 128 + half * 64, u * 128 + (half + 1) * 64)
                    o_buf[at] = acc_ref[at] + value[rows, v * 128:(v + 1) * 128]
            for half in range(2):
                out_copy(group, half).start()

    @pl.loop(0, 16)
    def _(group):
        for half in range(2):
            out_copy(group, half).wait()


def local(recorded, panels):
    tables, tails = jax.tree.map(jnp.asarray, lookup_tables())
    dma = pltpu.SemaphoreType.DMA
    whole = pl.BlockSpec(memory_space=pltpu.VMEM)
    acc, last = pl.pallas_call(
        kernel,
        out_shape=(pltpu.VMEM((128, 64, NT), F32), pltpu.VMEM((32, PITCH, 128), F32)),
        in_specs=[
            pl.BlockSpec(memory_space=pl.ANY),
            pl.BlockSpec(memory_space=pl.ANY),
            pl.BlockSpec(memory_space=pl.ANY),
        ],
        out_specs=(whole, whole),
        scratch_shapes=[
            pltpu.VMEM((6, 128, NT), BF16),
            pltpu.VMEM((128, 64, NT), F32),
            pltpu.VMEM((16, 64, NT), F32),
            pltpu.VMEM((8, 128, 128), F32),
            pltpu.VMEM((16, 8, 8, 128), F32),
            pltpu.VMEM((SLOTS, 16, 2, 2, 16, 512), F32),
            pltpu.VMEM((128, PITCH, 128), F32),
            pltpu.VMEM((SLOTS, 16, 2, 64, 128), F32),
            pltpu.VMEM((2, 256, 512), BF16),
            pltpu.VMEM((2, 256, 512), BF16),
            pltpu.VMEM((2, 512, 512), BF16),
            pltpu.VMEM((2, 512, 512), BF16),
            pltpu.VMEM((SLOTS, 16, 2, 64, 128), F32),
            pltpu.VMEM((SLOTS - 1, 32, PITCH, 128), F32),
            dma, dma((4, 2)), dma,
            dma((15,)), dma((15,)),
            dma((SLOTS, 15)), dma((SLOTS, 15)),
            dma((SLOTS, 15)), dma((SLOTS, 15)),
            dma((SLOTS, 4)), dma((SLOTS, 4)),
            dma((SLOTS, 3)), dma((SLOTS, 3)),
            dma((SLOTS, 8)), dma((SLOTS, 8)),
        ],
        compiler_params=pltpu.CompilerParams(
            collective_id=0, has_side_effects=True, vmem_limit_bytes=52 * 1024 * 1024
        ),
        name="convolve",
    )(recorded, panels, tables)
    return pl.pallas_call(
        finish,
        out_shape=jax.ShapeDtypeStruct((128, 64, NT), F32),
        in_specs=[whole, whole, whole, whole],
        out_specs=pl.BlockSpec(memory_space=pl.ANY),
        scratch_shapes=[pltpu.VMEM((128, 64, NT), F32), dma((16, 2))],
        compiler_params=pltpu.CompilerParams(vmem_limit_bytes=16 * 1024 * 1024),
        name="finish",
    )(acc, last.reshape(32 * PITCH, 128), *tails)


def solution(mesh):
    return jax.shard_map(
        local,
        mesh=mesh,
        in_specs=(P("src", "freq", None), P("src", "freq", None)),
        out_specs=P("src", "freq", None),
        check_vma=False,
    )
```

```python
import functools

import jax
import jax.numpy as jnp
import numpy as np
from jax import lax
from jax.experimental import pallas as pl
from jax.experimental.pallas import tpu as pltpu
from jax.sharding import PartitionSpec as P

NT = 128
NF = 64
SLOTS = 4
PITCH = 72
GROUPS = 8
MESH = pl.DeviceIdType.MESH
F32 = jnp.float32
BF16 = jnp.bfloat16

PLANE = [
    (1, 0), (0, 1), (3, 0), (0, 3), (1, 2), (2, 1), (3, 2), (2, 3),
    (1, 1), (3, 3), (2, 2), (1, 3), (3, 1), (2, 0), (0, 2),
]


def lookup_tables():
    phase = np.arange(NF)[:, None] * np.arange(NT)[None, :] % NT
    angle = 2.0 * np.pi / NT * phase
    forward = np.stack([np.cos(angle), -np.sin(angle)], axis=1)
    weight = np.where(np.arange(NF) == 0, 1.0, 2.0) / NT
    inverse = forward * weight[:, None, None]
    by_owner = forward.reshape(2 * NF, NT)
    forward, inverse = (
        table.reshape(16, SLOTS, 2, NT).transpose(1, 0, 2, 3).reshape(2 * NF, NT) for table in (forward, inverse)
    )
    tables = np.stack([part for table in (by_owner, forward, inverse) for part in split_table(table)])
    tail_hi, tail_lo = (np.kron(np.eye(4), part[96:].astype(np.float32)).astype(BF16) for part in tables[4:])
    return tables, (np.concatenate([tail_hi, tail_hi]), tail_lo)


def split_table(table):
    high = table.astype(np.float32).astype(BF16)
    low = (table - high.astype(np.float64)).astype(np.float32).astype(BF16)
    return high, low


def split(value):
    high = value.astype(BF16)
    return high, (value - high.astype(F32)).astype(BF16)


def halves(first, second):
    lane = lax.broadcasted_iota(jnp.int32, first.shape, first.ndim - 1)
    low = jnp.where(lane < 64, first, pltpu.roll(second, 64, axis=first.ndim - 1))
    high = jnp.where(lane < 64, pltpu.roll(first, 64, axis=first.ndim - 1), second)
    return low, high


def kernel(
    rec_hbm, pan_hbm, table_hbm, acc_ref, m_last,
    tables, x_buf, p_buf, g_send, g_recv, g_all, d_send, d_recv, d_hi, d_lo, g_hi, g_lo, m_send, m_recv,
    t_sem, x_sem, p_sem, gs_sem, gr_sem, ds_sem, dr_sem, ms_sem, mr_sem,
    fs_sem, fr_sem, bs_sem, br_sem, cs_sem, cr_sem,
):
    own_o = lax.axis_index("freq")
    src = lax.axis_index("src")
    own_xhi = src // 16
    zc = lax.rem(src, 16)
    z = zc // 2
    core = lax.rem(zc, 2)
    x = own_xhi * 2 + own_o // 4
    y = lax.rem(own_o, 4)
    own_q = own_xhi * 8 + own_o

    def plane(offset):
        px = lax.rem(x + offset[0], 4)
        py = lax.rem(y + offset[1], 4)
        o = lax.rem(px, 2) * 4 + py
        return o, px // 2

    def plane_id(offset):
        o, xhi = plane(offset)
        return (o, xhi * 16 + zc)

    step = 1 - 2 * core
    z_ahead = lax.rem(z + step + 8, 8)
    z_behind = lax.rem(z - step + 8, 8)
    ahead_id = (own_o, own_xhi * 16 + z_ahead * 2 + core)
    behind_id = (own_o, own_xhi * 16 + z_behind * 2 + core)
    partner_id = (own_o, own_xhi * 16 + z * 2 + 1 - core)

    pan_copy = pltpu.make_async_copy(pan_hbm, p_buf, p_sem)
    pan_copy.start()
    table_copy = pltpu.make_async_copy(table_hbm, tables, t_sem)
    table_copy.start()

    def rec_copy(chunk, half):
        rows = pl.ds(half * 64 + chunk * 16, 16)
        return pltpu.make_async_copy(rec_hbm.at[rows], x_buf.at[rows], x_sem.at[chunk, half])

    for chunk in range(4):
        for half in range(2):
            rec_copy(chunk, half).start()

    barrier = pltpu.get_barrier_semaphore()
    others = [plane_id(offset) for offset in PLANE] + [ahead_id, behind_id, partner_id]
    for other in others:
        pl.semaphore_signal(barrier, inc=1, device_id=other, device_id_type=MESH)

    nt = (((1,), (1,)), ((), ()))

    def forward(table, freqs, rows):
        high, low = split(rows)
        fwd_hi, fwd_lo = tables[table, freqs, :], tables[table + 1, freqs, :]
        return (
            lax.dot_general(fwd_hi, high, nt, preferred_element_type=F32)
            + lax.dot_general(fwd_hi, low, nt, preferred_element_type=F32)
            + lax.dot_general(fwd_lo, high, nt, preferred_element_type=F32)
        )

    pan_copy.wait()
    table_copy.wait()
    for kp in range(0, 8, 2):
        rows = jnp.concatenate([p_buf[kp], p_buf[kp + 8], p_buf[kp + 1], p_buf[kp + 9]], axis=0)
        hat = forward(0, slice(0, 128), rows)
        g_send[kp] = hat[:, :128]
        g_send[kp + 1] = hat[:, 128:]

    pl.semaphore_wait(barrier, len(others))

    def g_copy(n):
        o, xhi = plane(PLANE[n])
        return pltpu.make_async_remote_copy(
            src_ref=g_send.at[:, pl.ds((xhi * 8 + o) * 8, 8)],
            dst_ref=g_recv.at[own_q],
            send_sem=gs_sem.at[n], recv_sem=gr_sem.at[n],
            device_id=plane_id(PLANE[n]), device_id_type=MESH,
        )

    for n in range(15):
        g_copy(n).start()
    g_recv[own_q] = g_send[:, pl.ds(own_q * 8, 8), :]

    def d_copy(slot, n):
        o, xhi = plane(PLANE[n])
        return pltpu.make_async_remote_copy(
            src_ref=d_send.at[pl.ds(slot * 32 + (xhi * 8 + o) * 2, 2), pl.ds(0, 64)],
            dst_ref=d_recv.at[slot, own_q],
            send_sem=ds_sem.at[slot, n], recv_sem=dr_sem.at[slot, n],
            device_id=plane_id(PLANE[n]), device_id_type=MESH,
        )

    def spectra(start, count, ih):
        rows = jnp.concatenate([x_buf[ih], x_buf[ih + 64], x_buf[ih + 1], x_buf[ih + 65]], axis=0)
        freqs = slice(start, start + count)
        hat = forward(2, freqs, rows)
        d_send[freqs, ih, :] = hat[:, :128]
        d_send[freqs, ih + 1, :] = hat[:, 128:]

    def d_start(slot):
        for n in range(15):
            d_copy(slot, n).start()
        d_recv[slot, own_q] = d_send[pl.ds(slot * 32 + own_q * 2, 2), 0:64, :]

    for chunk in range(4):
        for half in range(2):
            rec_copy(chunk, half).wait()

        @pl.loop(0, 4)
        def _(quad):
            for u in range(2):
                spectra(0, 32, chunk * 16 + quad * 4 + u * 2)

    d_start(0)

    @pl.loop(0, 32)
    def _(pair):
        spectra(32, 96, pair * 2)

    @pl.loop(1, SLOTS)
    def _(slot):
        d_start(slot)

    for n in range(15):
        g_copy(n).wait_recv()

    @pl.loop(0, SLOTS)
    def _(slot):
        for c in range(2):
            row = slot * 2 + c
            for xhi in range(2):
                for pair in range(4):
                    low, high = halves(
                        g_recv[xhi * 8 + 2 * pair, :, row, :], g_recv[xhi * 8 + 2 * pair + 1, :, row, :]
                    )
                    g_all[slot, zc, c, xhi, 0:8, pair * 128:(pair + 1) * 128] = low
                    g_all[slot, zc, c, xhi, 8:16, pair * 128:(pair + 1) * 128] = high

    def block(hop, way):
        return lax.rem(z - way * hop * step + 32, 8) * 2 + core

    def ahead_copy(slot, hop):
        ref = g_all.at[slot, block(hop, 1)]
        return pltpu.make_async_remote_copy(
            src_ref=ref, dst_ref=ref, send_sem=fs_sem.at[slot, hop], recv_sem=fr_sem.at[slot, hop],
            device_id=ahead_id, device_id_type=MESH,
        )

    def behind_copy(slot, hop):
        ref = g_all.at[slot, block(hop, -1)]
        return pltpu.make_async_remote_copy(
            src_ref=ref, dst_ref=ref, send_sem=bs_sem.at[slot, hop], recv_sem=br_sem.at[slot, hop],
            device_id=behind_id, device_id_type=MESH,
        )

    def partner_copy(slot, n):
        ref = g_all.at[slot, block(n, 1) if n < 5 else block(n - 4, -1)]
        return pltpu.make_async_remote_copy(
            src_ref=ref, dst_ref=ref, send_sem=cs_sem.at[slot, n], recv_sem=cr_sem.at[slot, n],
            device_id=partner_id, device_id_type=MESH,
        )

    def first(slot):
        ahead_copy(slot, 0).start()
        behind_copy(slot, 0).start()
        partner_copy(slot, 0).start()

    def pass_on(hop, slot):
        ahead_copy(slot, hop).wait_recv()
        if hop < 3:
            ahead_copy(slot, hop + 1).start()
        partner_copy(slot, hop + 1).start()
        if hop < 3:
            behind_copy(slot, hop).wait_recv()
            if hop < 2:
                behind_copy(slot, hop + 1).start()
            partner_copy(slot, hop + 5).start()

    first(0)
    first(1)
    pass_on(0, 0)
    first(2)
    pass_on(1, 0)
    pass_on(0, 1)
    first(3)
    pass_on(2, 0)
    pass_on(1, 1)
    pass_on(0, 2)

    def m_copy(slot, n):
        o, xhi = plane(PLANE[n])
        if slot is None:
            slot, dst = SLOTS - 1, m_last
        else:
            dst = m_recv.at[slot]
        return pltpu.make_async_remote_copy(
            src_ref=m_send.at[slot, xhi * 8 + o],
            dst_ref=dst.at[pl.ds(own_q * 2, 2), pl.ds(0, 64)],
            send_sem=ms_sem.at[slot, n], recv_sem=mr_sem.at[slot, n],
            device_id=plane_id(PLANE[n]), device_id_type=MESH,
        )

    def dot(left, right):
        return jnp.dot(left, right, preferred_element_type=F32)

    def predict(slot):
        for n in range(8):
            partner_copy(slot, n).wait_recv()

        @pl.loop(0, 16)
        def _(b):
            for c in range(2):
                for xhi in range(2):
                    high, low = split(g_all[slot, b, c, xhi])
                    rows = pl.ds(xhi * 256 + b * 16, 16)
                    g_hi[c, rows, :] = high
                    g_lo[c, rows, :] = low

        for n in range(15):
            d_copy(slot, n).wait_recv()

        for xhi in range(2):
            for pair in range(4):
                for c in range(2):
                    top, bottom = halves(
                        d_recv[slot, xhi * 8 + 2 * pair, c], d_recv[slot, xhi * 8 + 2 * pair + 1, c]
                    )
                    for at, part in ((0, top), (64, bottom)):
                        high, low = split(part)
                        d_hi[c, xhi * 128 + at:xhi * 128 + at + 64, pair * 128:(pair + 1) * 128] = high
                        d_lo[c, xhi * 128 + at:xhi * 128 + at + 64, pair * 128:(pair + 1) * 128] = low

        @pl.loop(0, 2)
        def _(xhi):
            rows = pl.ds(xhi * 128, 128)
            for tile in range(2):
                cols = slice(tile * 256, (tile + 1) * 256)

                def product(a, b):
                    return (
                        dot(d_hi[a, rows, :], g_hi[b, :, cols])
                        + dot(d_hi[a, rows, :], g_lo[b, :, cols])
                        + dot(d_lo[a, rows, :], g_hi[b, :, cols])
                    )

                real = product(0, 0) - product(1, 1)
                imag = product(0, 1) + product(1, 0)
                for c, value in ((0, real), (1, imag)):
                    for lanes in range(2):
                        part = value[:, lanes * 128:(lanes + 1) * 128]
                        even, odd = halves(part[:64], part[64:])
                        o = tile * 4 + lanes * 2
                        m_send[slot, xhi * 8 + o, c] = even
                        m_send[slot, xhi * 8 + o + 1, c] = odd

    @pl.loop(0, SLOTS - 1)
    def _(slot):
        pass_on(3, slot)
        pass_on(2, slot + 1)

        @pl.when(slot < 2)
        def _():
            pass_on(1, slot + 2)

        @pl.when(slot < 1)
        def _():
            pass_on(0, slot + 3)

        predict(slot)
        for n in range(15):
            m_copy(slot, n).start()
        m_recv[slot, pl.ds(own_q * 2, 2), 0:64, :] = m_send[slot, own_q]

    pass_on(3, SLOTS - 1)
    predict(SLOTS - 1)
    for n in range(15):
        m_copy(None, n).start()
    m_last[pl.ds(own_q * 2, 2), 0:64, :] = m_send[SLOTS - 1, own_q]

    def arrive(slot):
        for n in range(15):
            m_copy(slot, n).wait_recv()

    def back(first, slots, ih):
        part = jnp.concatenate([m_recv[slot, :, ih, :] for slot in range(first, first + slots)], axis=0)
        high, low = split(part.T)
        freqs = slice(first * 32, (first + slots) * 32)
        inv_hi, inv_lo = tables[4, freqs, :], tables[5, freqs, :]
        return dot(high, inv_hi) + dot(low, inv_hi) + dot(high, inv_lo)

    arrive(0)
    arrive(1)

    @pl.loop(0, 32)
    def _(pair):
        for u in range(2):
            ih = pair * 2 + u
            value = back(0, 2, ih)
            acc_ref[ih] = value[:64]
            acc_ref[ih + 64] = value[64:]

    arrive(2)

    @pl.loop(0, 32)
    def _(pair):
        for u in range(2):
            ih = pair * 2 + u
            value = back(2, 1, ih)
            acc_ref[ih] += value[:64]
            acc_ref[ih + 64] += value[64:]

    for n in range(15):
        m_copy(None, n).wait_recv()

    for n in range(15):
        g_copy(n).wait_send()

    @pl.loop(0, SLOTS)
    def _(slot):
        for n in range(15):
            d_copy(slot, n).wait_send()
        for hop in range(4):
            ahead_copy(slot, hop).wait_send()
        for hop in range(3):
            behind_copy(slot, hop).wait_send()
        for n in range(8):
            partner_copy(slot, n).wait_send()

    @pl.loop(0, SLOTS - 1)
    def _(slot):
        for n in range(15):
            m_copy(slot, n).wait_send()

    for n in range(15):
        m_copy(None, n).wait_send()


def finish(acc_ref, m_last, tail_hi, tail_lo, out_hbm, o_buf, o_sem):
    def out_copy(group, half):
        rows = pl.ds(half * 64 + group * 4, 4)
        return pltpu.make_async_copy(o_buf.at[rows], out_hbm.at[rows], o_sem.at[group, half])

    @pl.loop(0, 16 // GROUPS)
    def _(step):
        parts = []
        for u in range(GROUPS):
            first = (step * GROUPS + u) * 4
            part = jnp.concatenate([m_last[pl.ds(first + v, 32, stride=PITCH), :] for v in range(4)], axis=0)
            parts.append(split(part.T))
        both = jnp.concatenate([jnp.concatenate(part, axis=1) for part in parts], axis=0)
        highs = jnp.concatenate([high for high, _ in parts], axis=0)
        value = jnp.dot(both, tail_hi[...], preferred_element_type=F32) + jnp.dot(
            highs, tail_lo[...], preferred_element_type=F32
        )
        for u in range(GROUPS):
            group = step * GROUPS + u
            for v in range(4):
                for half in range(2):
                    at = half * 64 + group * 4 + v
                    rows = slice(u * 128 + half * 64, u * 128 + (half + 1) * 64)
                    o_buf[at] = acc_ref[at] + value[rows, v * 128:(v + 1) * 128]
            for half in range(2):
                out_copy(group, half).start()

    @pl.loop(0, 16)
    def _(group):
        for half in range(2):
            out_copy(group, half).wait()


def local(recorded, panels):
    tables, tails = jax.tree.map(jnp.asarray, lookup_tables())
    dma = pltpu.SemaphoreType.DMA
    whole = pl.BlockSpec(memory_space=pltpu.VMEM)
    acc, last = pl.pallas_call(
        kernel,
        out_shape=(pltpu.VMEM((128, 64, NT), F32), pltpu.VMEM((32, PITCH, 128), F32)),
        in_specs=[
            pl.BlockSpec(memory_space=pl.ANY),
            pl.BlockSpec(memory_space=pl.ANY),
            pl.BlockSpec(memory_space=pl.ANY),
        ],
        out_specs=(whole, whole),
        scratch_shapes=[
            pltpu.VMEM((6, 128, NT), BF16),
            pltpu.VMEM((128, 64, NT), F32),
            pltpu.VMEM((16, 64, NT), F32),
            pltpu.VMEM((8, 128, 128), F32),
            pltpu.VMEM((16, 8, 8, 128), F32),
            pltpu.VMEM((SLOTS, 16, 2, 2, 16, 512), F32),
            pltpu.VMEM((128, PITCH, 128), F32),
            pltpu.VMEM((SLOTS, 16, 2, 64, 128), F32),
            pltpu.VMEM((2, 256, 512), BF16),
            pltpu.VMEM((2, 256, 512), BF16),
            pltpu.VMEM((2, 512, 512), BF16),
            pltpu.VMEM((2, 512, 512), BF16),
            pltpu.VMEM((SLOTS, 16, 2, 64, 128), F32),
            pltpu.VMEM((SLOTS - 1, 32, PITCH, 128), F32),
            dma, dma((4, 2)), dma,
            dma((15,)), dma((15,)),
            dma((SLOTS, 15)), dma((SLOTS, 15)),
            dma((SLOTS, 15)), dma((SLOTS, 15)),
            dma((SLOTS, 4)), dma((SLOTS, 4)),
            dma((SLOTS, 3)), dma((SLOTS, 3)),
            dma((SLOTS, 8)), dma((SLOTS, 8)),
        ],
        compiler_params=pltpu.CompilerParams(
            collective_id=0, has_side_effects=True, vmem_limit_bytes=52 * 1024 * 1024
        ),
        name="convolve",
    )(recorded, panels, tables)
    return pl.pallas_call(
        finish,
        out_shape=jax.ShapeDtypeStruct((128, 64, NT), F32),
        in_specs=[whole, whole, whole, whole],
        out_specs=pl.BlockSpec(memory_space=pl.ANY),
        scratch_shapes=[pltpu.VMEM((128, 64, NT), F32), dma((16, 2))],
        compiler_params=pltpu.CompilerParams(vmem_limit_bytes=16 * 1024 * 1024),
        name="finish",
    )(acc, last.reshape(32 * PITCH, 128), *tails)


def solution(mesh):
    return jax.shard_map(
        local,
        mesh=mesh,
        in_specs=(P("src", "freq", None), P("src", "freq", None)),
        out_specs=P("src", "freq", None),
        check_vma=False,
    )
```
